32 devices in a mesh: grp: 8 (over z, y), rep: 4 (over x, core).
Axes of the slice: x: 2, y: 2, z: 4, core: 2. Of those that a mesh axis runs over, the one named last changes fastest.
Arguments:
- queries: bfloat16 [16, 4, 32, 128], P('grp', 'rep'), may hold values from -3.2 to 3.2
- passages: bfloat16 [512, 4, 180, 128], P('grp', 'rep'), may hold values from -1.796875 to 1.796875
- lengths: int32 [512, 4], P('grp', 'rep'), may hold values from 16 to 180
- cand_ids: int32 [16, 4, 64], P('grp', 'rep'), may hold values from 0 to 511, as said below
- owner_map: int32 [4, 512], P('rep'), may hold values from 0 to 511, as said below
- teacher: float32 [16, 4, 64], P('grp', 'rep'), may hold values from -12 to 312
- weights: float32 [16, 4], P('grp', 'rep'), may hold values from 0.5 to 18
Outputs:
- loss: float32 [], replicated
- query_grad: float32 [16, 4, 32, 128], P('grp', 'rep')
- passage_grad: bfloat16 [512, 4, 180, 128], P('grp', 'rep')
The draws below stay inside these ranges and needn't reach their ends.
Inputs may be any that keep to these rules, and one draw needn't show every extreme that they name: `cand_ids`: within each replica, the 128 candidates of the queries of one grp index have storage rows of which at most 32 (counted with repeats) lie in any one aligned block of 64 rows; in every draw, in each replica, one block receives exactly 32 from every grp index. `owner_map`: each row is a permutation of 0 to 511.
All inputs are finite; a program needn't handle non-finite values.
Results may differ from the reference program's by a relative error of at most 0.0055.
Values may be sent and summed in bfloat16 or wider, within the bound.
A program may use at most 128 MiB of HBM per device.

```python
import math
import jax
import jax.numpy as jnp
from jax import lax

DIM = 128
QL = 32
PL = 180
NWAY = 64
Q_DEV = 2
P_DEV = 64
GROUPS = 8
REPS = 4
QUERIES = 16
PASSAGES = 512


def routing(key):
    ref_count = Q_DEV * NWAY
    capacity = 2 * ref_count // GROUPS
    pool_size = GROUPS * capacity
    keys = jax.random.split(jax.random.fold_in(key, 7), 5)
    hot_owner = jax.random.randint(keys[0], (REPS,), 0, GROUPS)
    pool_owner = jnp.arange(pool_size, dtype=jnp.int32) // capacity
    priority = jax.random.randint(keys[1], (GROUPS, REPS, pool_size), 0, 1 << 20) * pool_size + jnp.arange(pool_size, dtype=jnp.int32)
    is_hot = pool_owner[None, None, :] == hot_owner[None, :, None]
    priority = jnp.where(is_hot, jnp.arange(pool_size, dtype=jnp.int32) - pool_size, priority)
    order = jnp.argsort(priority, axis=-1)[..., :ref_count]
    owners = pool_owner[order]
    shuffle_key = jax.random.randint(keys[2], (GROUPS, REPS, ref_count), 0, 1 << 20) * ref_count + jnp.arange(ref_count, dtype=jnp.int32)
    shuffle = jnp.argsort(shuffle_key, axis=-1)
    owners = jnp.take_along_axis(owners, shuffle, axis=-1)
    slot_rows = jax.random.randint(keys[3], (GROUPS, REPS, ref_count), 0, P_DEV)
    storage = owners * P_DEV + slot_rows
    perm_keys = jax.random.split(keys[4], REPS)
    owner_table = jax.vmap(lambda one_key: jax.random.permutation(one_key, P_DEV * GROUPS))(perm_keys).astype(jnp.int32)
    inverse = jnp.argsort(owner_table, axis=-1).astype(jnp.int32)
    wide_inverse = jnp.broadcast_to(inverse[None], (GROUPS, REPS, P_DEV * GROUPS))
    identity = jnp.take_along_axis(wide_inverse, storage, axis=-1)
    candidate_ids = identity.reshape(GROUPS, REPS, Q_DEV, NWAY).transpose(0, 2, 1, 3).reshape(GROUPS * Q_DEV, REPS, NWAY)
    return (candidate_ids.astype(jnp.int32), owner_table)


def draw_cand_ids(key, part):
    return routing(key)[0]


def draw_owner_map(key, part):
    return routing(key)[1]


def draw_queries(key, part):
    keys = jax.random.split(jax.random.fold_in(key, 11), 2)
    shape = (QUERIES, REPS, QL, DIM)
    normal_part = jnp.clip(jax.random.normal(keys[0], shape, jnp.float32), -3.5, 3.5)
    row_scale = jnp.exp(jax.random.uniform(keys[1], (QUERIES, REPS, 1, 1), jnp.float32, math.log(0.03), math.log(3.0)))
    return (0.3 * normal_part * row_scale).astype(jnp.bfloat16)


def draw_teacher(key, part):
    keys = jax.random.split(jax.random.fold_in(key, 13), 1)
    normal_part = 2.0 * jnp.clip(jax.random.normal(keys[0], (QUERIES, REPS, NWAY), jnp.float32), -6.0, 6.0)
    return normal_part


def draw_weights(key, part):
    keys = jax.random.split(jax.random.fold_in(key, 17), 1)
    query_index = jnp.arange(QUERIES, dtype=jnp.int32)[:, None]
    replica_index = jnp.arange(REPS, dtype=jnp.int32)[None, :]
    device_index = query_index // Q_DEV * REPS + replica_index
    ramp = 1.0 + 2.0 * device_index.astype(jnp.float32) / (GROUPS * REPS - 1)
    return jnp.exp(jax.random.uniform(keys[0], (QUERIES, REPS), jnp.float32, math.log(0.5), math.log(2.0))) * ramp


def place_ends(values, stream_key, low, largest):
    longest = values.shape.index(max(values.shape))
    spots = []
    for shift in (0, 1):
        where = [jax.random.randint(jax.random.fold_in(stream_key, axis), (), 0, length) for axis, length in enumerate(values.shape)]
        where[longest] = (where[longest] + shift) % values.shape[longest]
        spots.append(tuple(where))
    return values.at[spots[0]].set(low).at[spots[1]].set(largest)


def block_levels(key, shape, pieces, low, top_value):
    loudness = 1.0
    for position, shards_of in pieces:
        heights = jax.random.uniform(jax.random.fold_in(jax.random.fold_in(key, 6), position), (shards_of,), jnp.float32, low / len(pieces), top_value / len(pieces))
        loudness = loudness * jnp.repeat(jnp.exp(heights), shape[position] // shards_of).reshape((-1,) + (1,) * (len(shape) - 1 - position))
    return loudness


def gaussian(rng, extent, width, bound, shards=(), held_as=jnp.bfloat16):
    entries = width * jax.random.normal(rng, extent, jnp.float32)
    if shards:
        entries = entries * block_levels(rng, extent, shards, -0.22, 0.18)
    return jnp.clip(entries, -bound, bound).astype(held_as)


def setup_inputs(seed: int = 0) -> dict:
    seeds = jax.random.split(jax.random.key(seed), 8)
    return {
        "queries": draw_queries(jax.random.fold_in(seeds[7], 71), 0),
        "passages": gaussian(seeds[1], (PASSAGES, REPS, PL, DIM), 0.3, 1.796875, ((0, 8), (1, 4))),
        "lengths": place_ends(jax.random.randint(seeds[2], (PASSAGES, REPS), 16, PL + 1), jax.random.fold_in(seeds[2], 1), 16, PL).astype(jnp.int32),
        "cand_ids": draw_cand_ids(jax.random.fold_in(seeds[7], 71), 0),
        "owner_map": draw_owner_map(jax.random.fold_in(seeds[7], 71), 0),
        "teacher": draw_teacher(jax.random.fold_in(seeds[7], 71), 0),
        "weights": draw_weights(jax.random.fold_in(seeds[7], 71), 0),
    }


temper = 0.05


def rounded(values):
    return lax.optimization_barrier(values.astype(jnp.bfloat16)).astype(jnp.float32)


def token_softmax(products, lengths_used):
    usable = lax.broadcasted_iota(jnp.int32, products.shape, products.ndim - 1) < lengths_used[..., None, None]
    scaled = jnp.where(usable, products / temper, -1e30)
    highest = jnp.max(scaled, axis=-1, keepdims=True)
    powers = jnp.where(usable, jnp.exp(scaled - highest), 0.0)
    summed = jnp.sum(powers, axis=-1, keepdims=True)
    matched = temper * (highest[..., 0] + jnp.log(summed[..., 0]))
    return matched, powers / summed


def pair_terms(query_tokens, passage_tokens, lengths_used):
    products = jnp.einsum("id,cjd->cij", query_tokens.astype(jnp.float32), passage_tokens.astype(jnp.float32))
    matched, attention = token_softmax(products, lengths_used)
    return jnp.sum(matched, axis=-1), attention


def reference(queries, passages, lengths, cand_ids, owner_map, teacher, weights):
    query_count = queries.shape[0]
    replicas = queries.shape[1]

    def fetch_blocks(query_row, replica):
        storage_rows = owner_map[replica][cand_ids[query_row, replica]]
        return storage_rows, passages[storage_rows, replica], lengths[storage_rows, replica]

    def score_one(flat_index):
        query_row = flat_index // replicas
        replica = flat_index % replicas
        storage_rows, blocks, lengths_used = fetch_blocks(query_row, replica)
        return pair_terms(queries[query_row, replica], blocks, lengths_used)[0]

    student = lax.map(score_one, jnp.arange(query_count * replicas, dtype=jnp.int32))
    student = student.reshape(query_count, replicas, -1)
    log_student = jax.nn.log_softmax(student, axis=-1)
    log_teacher = jax.nn.log_softmax(teacher, axis=-1)
    teacher_prob = jnp.exp(log_teacher)
    divergence = jnp.sum(teacher_prob * (log_teacher - log_student), axis=-1)
    weight_sum = jnp.sum(weights)
    loss_value = jnp.sum(weights * divergence) / weight_sum
    score_grad = (query_count * replicas) * weights[..., None] / weight_sum * (jnp.exp(log_student) - teacher_prob)
    query_parts = []
    passage_parts = []
    for replica in range(replicas):
        def backward(accum_grad, query_row):
            storage_rows, blocks, lengths_used = fetch_blocks(query_row, replica)
            query_tokens = queries[query_row, replica]
            unused, attention = pair_terms(query_tokens, blocks, lengths_used)
            scaled_grad = rounded(score_grad[query_row, replica][:, None, None] * attention)
            pair_query = rounded(jnp.einsum("cij,cjd->cid", scaled_grad, blocks.astype(jnp.float32)))
            query_part = jnp.sum(pair_query, axis=0)
            pair_passage = rounded(jnp.einsum("cij,id->cjd", scaled_grad, query_tokens.astype(jnp.float32)))
            accum_grad = accum_grad.at[storage_rows].add(pair_passage)
            return accum_grad, query_part

        initial = jnp.zeros((passages.shape[0],) + passages.shape[2:], jnp.float32)
        summed, replica_grads = lax.scan(backward, initial, jnp.arange(query_count, dtype=jnp.int32))
        query_parts.append(replica_grads)
        passage_parts.append(summed.astype(jnp.bfloat16))
    return loss_value, jnp.stack(query_parts, axis=1), jnp.stack(passage_parts, axis=1)
```

```python
import functools
import math

import jax
import jax.numpy as jnp
from jax import lax
from jax.experimental import pallas as pl
from jax.experimental.pallas import tpu as pltpu
from jax.sharding import PartitionSpec as P

temper = 0.05
to_base2 = 1.0 / (temper * math.log(2.0))
LANES = 128
MESH = pl.DeviceIdType.MESH
HIGH = lax.Precision.HIGHEST
VMEM_SPEC = pl.BlockSpec(memory_space=pltpu.VMEM)


def greet(groups, replicas, me, mine):
    barrier = pltpu.get_barrier_semaphore()
    for step in range(1, groups):
        pl.semaphore_signal(
            barrier, inc=1, device_id={"grp": lax.rem(me + step, groups)}, device_id_type=MESH
        )
    for step in range(1, replicas):
        pl.semaphore_signal(
            barrier, inc=1, device_id={"rep": lax.rem(mine + step, replicas)}, device_id_type=MESH
        )


def greeted(groups, replicas):
    pl.semaphore_wait(pltpu.get_barrier_semaphore(), groups - 1 + replicas - 1)


def share_kernel(
    groups, block, queries_ref, cand_ref, map_ref, teacher_ref, weights_ref,
    all_queries, all_meta, query_buf, meta_buf, send_sem, recv_sem,
):
    me = lax.axis_index("grp")
    greet(groups, 1, me, 0)
    count, ways = cand_ref.shape
    table = map_ref[...].astype(jnp.float32)
    ids = lax.broadcasted_iota(jnp.int32, (ways, table.shape[1]), 1)
    diagonal = lax.broadcasted_iota(jnp.int32, (ways, ways), 0) == lax.broadcasted_iota(
        jnp.int32, (ways, ways), 1
    )
    teacher = teacher_ref[...]
    top = jnp.max(teacher, axis=1, keepdims=True)
    log_teacher = teacher - top
    log_teacher = log_teacher - jnp.log(jnp.sum(jnp.exp(log_teacher), axis=1, keepdims=True))
    prob = jnp.exp(log_teacher)
    entropy = jnp.sum(prob * log_teacher, axis=1, keepdims=True)
    meta_buf[me] = jnp.zeros(meta_buf.shape[1:], jnp.float32)
    for q in range(count):
        line = cand_ref[q : q + 1, :].astype(jnp.float32)
        column = jnp.sum(jnp.where(diagonal, line, 0.0), axis=1, keepdims=True).astype(jnp.int32)
        row = jnp.sum(jnp.where(column == ids, table, 0.0), axis=1, keepdims=True)
        row = jnp.sum(jnp.where(diagonal, row, 0.0), axis=0, keepdims=True)
        meta_buf[me, q : q + 1, :ways] = row
    meta_buf[me, count : 2 * count, :ways] = prob
    for q in range(count):
        meta_buf[me, 2 * count + q : 2 * count + q + 1, :] = jnp.broadcast_to(
            weights_ref[:, q : q + 1], (1, LANES)
        )
    meta_buf[me, 3 * count : 4 * count, :] = jnp.broadcast_to(entropy, (count, LANES))
    query_buf[me] = queries_ref[...]
    greeted(groups, 1)
    copies = []
    for step in range(1, groups):
        peer = lax.rem(me + step, groups)
        for which, buf in enumerate((query_buf, meta_buf)):
            copies.append(
                pltpu.make_async_remote_copy(
                    src_ref=buf.at[me],
                    dst_ref=buf.at[me],
                    send_sem=send_sem.at[which, step],
                    recv_sem=recv_sem.at[which, step],
                    device_id={"grp": peer},
                    device_id_type=MESH,
                )
            )
            copies[-1].start()
    for copy in copies:
        copy.wait()
    all_queries[...] = query_buf[...]
    all_meta[...] = meta_buf[...]


def span_of(tokens, limit):
    return max(size for size in range(1, limit + 1) if tokens % size == 0)


def lengths_of(lengths_ref, first, rows, width):
    index = lax.broadcasted_iota(jnp.int32, (rows, width), 0)
    found = jnp.zeros((rows, width), jnp.int32)
    for k in range(rows):
        found = jnp.where(index == k, lengths_ref[first + k], found)
    return found


def forward_kernel(
    count, ways, block, lengths_ref, passages_ref, queries_ref, meta_ref,
    lse_ref, score_ref, hits_ref, mass_ref, held, all_lse,
):
    step = pl.program_id(0)
    part = pl.program_id(1)
    groups = meta_ref.shape[0]
    tokens, rows, dim = passages_ref.shape
    width = queries_ref.shape[0]
    slot = score_ref.shape[1]

    @pl.when((step == 0) & (part == 0))
    def _():
        spots = lax.broadcasted_iota(jnp.int32, (ways, groups * slot), 1)
        for source in range(groups):
            turned = jnp.transpose(meta_ref[source])
            for q in range(count):
                row = turned[:ways, q : q + 1].astype(jnp.int32)
                spot = row + (slot - block) * (row // block)
                hot = spot == spots
                place = source * count + q
                hits_ref[place : place + 1, :] = jnp.sum(
                    jnp.where(hot, 1.0, 0.0), axis=0, keepdims=True
                )
                mass_ref[place : place + 1, :] = jnp.sum(
                    jnp.where(hot, turned[:ways, count + q : count + q + 1], 0.0),
                    axis=0,
                    keepdims=True,
                )

    lengths = lengths_of(lengths_ref, step * rows, rows, width)
    size = span_of(tokens, 20)
    highest = jnp.full((rows, width), -1e30, jnp.float32)
    for first in range(0, tokens, size):
        products = lax.dot_general(
            passages_ref[first : first + size].reshape(size * rows, dim), queries_ref[...],
            (((1,), (1,)), ((), ())), preferred_element_type=jnp.float32,
        )
        for j in range(size):
            scaled = jnp.where(
                first + j < lengths, products[j * rows : (j + 1) * rows] * to_base2, -1e30
            )
            held[first + j] = scaled
            highest = jnp.maximum(highest, scaled)
    summed = jnp.zeros((rows, width), jnp.float32)
    for j in range(tokens):
        summed = summed + jnp.exp2(held[j] - highest)
    lse = highest + jnp.log2(summed)
    lse_ref[...] = lse
    all_lse[step, part] = lse

    @pl.when((step == pl.num_programs(0) - 1) & (part == pl.num_programs(1) - 1))
    def _():
        total = score_ref.shape[0]
        parts = all_lse.shape[1]
        each = width * parts // total
        score_ref[...] = jnp.zeros_like(score_ref)
        belongs = lax.broadcasted_iota(jnp.int32, (total // parts, width), 1) // each
        pick = jnp.where(
            belongs == lax.broadcasted_iota(jnp.int32, (total // parts, width), 0), 1.0, 0.0
        )
        span = total // parts
        for k in range(parts):
            matched = jnp.concatenate(
                [all_lse[i, k] for i in range(all_lse.shape[0])], axis=0
            ) * (1.0 / to_base2)
            score_ref[k * span : (k + 1) * span, :block] = lax.dot_general(
                pick, matched, (((1,), (1,)), ((), ())),
                precision=HIGH, preferred_element_type=jnp.float32,
            )


def grade_kernel(
    groups, replicas, score_ref, hits_ref, mass_ref, meta_ref, grad_ref, loss_ref,
    score_buf, weight_buf, grad_buf, query_weight, query_entropy,
    send_sem, recv_sem, wsend_sem, wrecv_sem,
):
    me = lax.axis_index("grp")
    mine = lax.axis_index("rep")
    greet(groups, replicas, me, mine)
    total, slot = score_ref.shape
    count = total // groups
    for source in range(groups):
        span = slice(source * count, (source + 1) * count)
        query_weight[span, :] = meta_ref[source, 2 * count : 3 * count, :]
        query_entropy[span, :] = meta_ref[source, 3 * count : 4 * count, :]
    weights = query_weight[:, :1]
    score_buf[me] = score_ref[...]
    weight_buf[mine] = jnp.broadcast_to(
        jnp.sum(query_weight[...], axis=0, keepdims=True), weight_buf.shape[1:]
    )
    greeted(groups, replicas)
    copies = []
    for step in range(1, groups):
        copies.append(
            pltpu.make_async_remote_copy(
                src_ref=score_buf.at[me],
                dst_ref=score_buf.at[me],
                send_sem=send_sem.at[step],
                recv_sem=recv_sem.at[step],
                device_id={"grp": lax.rem(me + step, groups)},
                device_id_type=MESH,
            )
        )
        copies[-1].start()
    for step in range(1, replicas):
        copies.append(
            pltpu.make_async_remote_copy(
                src_ref=weight_buf.at[mine],
                dst_ref=weight_buf.at[mine],
                send_sem=wsend_sem.at[step],
                recv_sem=wrecv_sem.at[step],
                device_id={"rep": lax.rem(mine + step, replicas)},
                device_id_type=MESH,
            )
        )
        copies[-1].start()
    for copy in copies:
        copy.wait()
    weight_sum = jnp.sum(weight_buf[...], axis=0)[:1, :1]
    scores = jnp.concatenate([score_buf[owner] for owner in range(groups)], axis=1)
    hits = hits_ref[...]
    mass = mass_ref[...]
    asked = hits > 0.0
    held = jnp.where(asked, scores, -1e30)
    highest = jnp.max(held, axis=1, keepdims=True)
    summed = jnp.sum(hits * jnp.exp(held - highest), axis=1, keepdims=True)
    log_student = jnp.where(asked, scores - (highest + jnp.log(summed)), -1e30)
    student = hits * jnp.exp(log_student)
    crossed = jnp.sum(jnp.where(asked, mass * log_student, 0.0), axis=1, keepdims=True)
    divergence = query_entropy[:, :1] - crossed
    grad_buf[...] = (total * replicas) * weights / weight_sum * (student - mass)
    own = grad_buf[:, pl.ds(pl.multiple_of(me * slot, slot), slot)]
    width = grad_ref.shape[1]
    each = width // total
    belongs = lax.broadcasted_iota(jnp.int32, (total, width), 1) // each
    pick = jnp.where(belongs == lax.broadcasted_iota(jnp.int32, (total, width), 0), 1.0, 0.0)
    spread = lax.dot_general(
        own, pick, (((0,), (0,)), ((), ())), precision=HIGH, preferred_element_type=jnp.float32
    )
    grad_ref[...] = spread[: grad_ref.shape[0]]
    loss_ref[...] = jnp.broadcast_to(
        jnp.sum(weights * divergence, axis=0, keepdims=True) / weight_sum, loss_ref.shape
    )


def backward_kernel(
    lengths_ref, passages_ref, queries_ref, lse_ref, grad_ref, out_ref, partial_ref,
    total, token_total,
):
    step = pl.program_id(0)
    part = pl.program_id(1)
    parts = total.shape[0]
    tokens, rows, dim = passages_ref.shape
    width = queries_ref.shape[0]

    @pl.when(step == 0)
    def _():
        total[part] = jnp.zeros(total.shape[1:], jnp.float32)

    if parts > 1:

        @pl.when(part == 0)
        def _():
            token_total[...] = jnp.zeros_like(token_total)

    lengths = lengths_of(lengths_ref, step * rows, rows, width)[None]
    lse = lse_ref[...][None]
    grad = grad_ref[...][None]
    queries = queries_ref[...]
    size = span_of(tokens, 36)
    added = None
    for first in range(0, tokens, size):
        passage = passages_ref[first : first + size].reshape(size * rows, dim)
        products = lax.dot_general(
            passage, queries, (((1,), (1,)), ((), ())), preferred_element_type=jnp.float32
        ).reshape(size, rows, width)
        position = first + lax.broadcasted_iota(jnp.int32, (size, 1, 1), 0)
        powers = jnp.exp2(jnp.where(position < lengths, products * to_base2 - lse, -1e30))
        scaled_grad = (powers * grad).astype(jnp.bfloat16).reshape(size * rows, width)
        token_grad = jnp.dot(scaled_grad, queries, preferred_element_type=jnp.float32).reshape(
            size, rows, dim
        )
        if parts > 1:
            token_total[first : first + size] += token_grad
        else:
            out_ref[first : first + size] = token_grad.astype(jnp.bfloat16)
        piece = lax.dot_general(
            passage, scaled_grad, (((0,), (0,)), ((), ())), preferred_element_type=jnp.float32
        )
        added = piece if added is None else added + piece
    total[part] += added

    if parts > 1:

        @pl.when(part == parts - 1)
        def _():
            out_ref[...] = token_total[...].astype(jnp.bfloat16)

    @pl.when(step == pl.num_programs(0) - 1)
    def _():
        partial_ref[pl.ds(pl.multiple_of(part * width, width), width), :] = jnp.transpose(
            total[part]
        ).astype(partial_ref.dtype)


def collect_kernel(
    groups, replicas, partial_ref, loss_ref, grad_ref, loss_out,
    arrived, loss_buf, send_sem, recv_sem, lsend_sem, lrecv_sem,
):
    me = lax.axis_index("grp")
    mine = lax.axis_index("rep")
    greet(groups, replicas, me, mine)
    loss_buf[mine] = loss_ref[...]
    greeted(groups, replicas)
    copies = []
    for step in range(1, groups):
        peer = lax.rem(me + step, groups)
        copies.append(
            pltpu.make_async_remote_copy(
                src_ref=partial_ref.at[peer],
                dst_ref=arrived.at[me],
                send_sem=send_sem.at[step],
                recv_sem=recv_sem.at[step],
                device_id={"grp": peer},
                device_id_type=MESH,
            )
        )
        copies[-1].start()
    for step in range(1, replicas):
        copies.append(
            pltpu.make_async_remote_copy(
                src_ref=loss_buf.at[mine],
                dst_ref=loss_buf.at[mine],
                send_sem=lsend_sem.at[step],
                recv_sem=lrecv_sem.at[step],
                device_id={"rep": lax.rem(mine + step, replicas)},
                device_id_type=MESH,
            )
        )
        copies[-1].start()
    arrived[me] = partial_ref[me]
    for copy in copies:
        copy.wait()
    grad_ref[...] = jnp.sum(arrived[...].astype(jnp.float32), axis=0)
    loss_out[...] = jnp.sum(loss_buf[...], axis=0)[:1, :1]


def on_device(queries, passages, lengths, cand_ids, owner_map, teacher, weights):
    groups = lax.axis_size("grp")
    replicas = lax.axis_size("rep")
    count, _, query_len, dim = queries.shape
    block, _, tokens, _ = passages.shape
    ways = cand_ids.shape[2]
    own_rows = count * query_len
    width = groups * own_rows
    total = groups * count
    slot = -(-block // LANES) * LANES
    f32 = jnp.float32
    dma = pltpu.SemaphoreType.DMA
    meta_rows = -(-4 * count // 8) * 8
    all_queries, all_meta = pl.pallas_call(
        functools.partial(share_kernel, groups, block),
        name="share",
        out_shape=[
            jax.ShapeDtypeStruct((groups, own_rows, dim), queries.dtype),
            jax.ShapeDtypeStruct((groups, meta_rows, LANES), f32),
        ],
        in_specs=[VMEM_SPEC] * 5,
        out_specs=[VMEM_SPEC] * 2,
        scratch_shapes=[
            pltpu.VMEM((groups, own_rows, dim), queries.dtype),
            pltpu.VMEM((groups, meta_rows, LANES), f32),
            dma((2, groups)),
            dma((2, groups)),
        ],
        compiler_params=pltpu.CompilerParams(collective_id=0, has_side_effects=True),
    )(
        queries.reshape(own_rows, dim),
        cand_ids[:, 0],
        owner_map,
        teacher[:, 0],
        jnp.transpose(weights),
    )
    flat_queries = all_queries.reshape(width, dim)
    flat_passages = jnp.transpose(passages[:, 0], (1, 0, 2))
    flat_lengths = lengths.reshape(block)
    rows = 16 if block % 16 == 0 else block
    chunk = width if width <= 512 else width // (width // 512)
    parts = width // chunk
    grid = (block // rows, parts)
    whole = lambda *shape: pl.BlockSpec(shape, lambda i, k, *_: (0,) * len(shape))
    passage_spec = pl.BlockSpec((tokens, rows, dim), lambda i, k, *_: (0, i, 0))
    query_spec = pl.BlockSpec((chunk, dim), lambda i, k, *_: (k, 0))
    row_spec = pl.BlockSpec((rows, chunk), lambda i, k, *_: (i, k))
    both = pltpu.CompilerParams(dimension_semantics=("arbitrary", "arbitrary"))
    lse, score, hits, mass = pl.pallas_call(
        functools.partial(forward_kernel, count, ways, block),
        name="forward",
        grid_spec=pltpu.PrefetchScalarGridSpec(
            num_scalar_prefetch=1,
            grid=grid,
            in_specs=[passage_spec, query_spec, whole(groups, meta_rows, LANES)],
            out_specs=[
                row_spec,
                whole(total, slot),
                whole(total, groups * slot),
                whole(total, groups * slot),
            ],
            scratch_shapes=[
                pltpu.VMEM((tokens, rows, chunk), f32),
                pltpu.VMEM((*grid, rows, chunk), f32),
            ],
        ),
        out_shape=[
            jax.ShapeDtypeStruct((block, width), f32),
            jax.ShapeDtypeStruct((total, slot), f32),
            jax.ShapeDtypeStruct((total, groups * slot), f32),
            jax.ShapeDtypeStruct((total, groups * slot), f32),
        ],
        compiler_params=both,
    )(flat_lengths, flat_passages, flat_queries, all_meta)
    grad, loss_part = pl.pallas_call(
        functools.partial(grade_kernel, groups, replicas),
        name="grade",
        out_shape=[
            jax.ShapeDtypeStruct((block, width), f32),
            jax.ShapeDtypeStruct((8, LANES), f32),
        ],
        in_specs=[VMEM_SPEC] * 4,
        out_specs=[VMEM_SPEC] * 2,
        scratch_shapes=[
            pltpu.VMEM((groups, total, slot), f32),
            pltpu.VMEM((replicas, 8, LANES), f32),
            pltpu.VMEM((total, groups * slot), f32),
            pltpu.VMEM((total, LANES), f32),
            pltpu.VMEM((total, LANES), f32),
            dma((groups,)),
            dma((groups,)),
            dma((replicas,)),
            dma((replicas,)),
        ],
        compiler_params=pltpu.CompilerParams(collective_id=1, has_side_effects=True),
    )(score, hits, mass, all_meta)
    passage_grad, partial = pl.pallas_call(
        backward_kernel,
        name="backward",
        grid_spec=pltpu.PrefetchScalarGridSpec(
            num_scalar_prefetch=1,
            grid=grid,
            in_specs=[passage_spec, query_spec, row_spec, row_spec],
            out_specs=[passage_spec, whole(width, dim)],
            scratch_shapes=[
                pltpu.VMEM((parts, dim, chunk), f32),
                pltpu.VMEM((tokens, rows, dim) if parts > 1 else (8, rows, dim), f32),
            ],
        ),
        out_shape=[
            jax.ShapeDtypeStruct((tokens, block, dim), jnp.bfloat16),
            jax.ShapeDtypeStruct((width, dim), jnp.bfloat16),
        ],
        compiler_params=both,
    )(flat_lengths, flat_passages, flat_queries, lse, grad)
    query_grad, loss = pl.pallas_call(
        functools.partial(collect_kernel, groups, replicas),
        name="collect",
        out_shape=[
            jax.ShapeDtypeStruct((own_rows, dim), f32),
            jax.ShapeDtypeStruct((1, 1), f32),
        ],
        in_specs=[VMEM_SPEC] * 2,
        out_specs=[VMEM_SPEC] * 2,
        scratch_shapes=[
            pltpu.VMEM((groups, own_rows, dim), jnp.bfloat16),
            pltpu.VMEM((replicas, 8, LANES), f32),
            dma((groups,)),
            dma((groups,)),
            dma((replicas,)),
            dma((replicas,)),
        ],
        compiler_params=pltpu.CompilerParams(collective_id=2, has_side_effects=True),
    )(partial.reshape(groups, own_rows, dim), loss_part)
    return (
        loss.reshape(()),
        query_grad.reshape(count, 1, query_len, dim),
        jnp.transpose(passage_grad, (1, 0, 2))[:, None],
    )


def partner(me, turn):
    peer = me
    bit = 1
    while bit <= turn:
        if turn & bit:
            peer = peer + bit * (1 - 2 * lax.rem(lax.div(me, bit), 2))
        bit *= 2
    return peer


def share_meta(me, cand, table, teacher, weights, meta_buf):
    count, ways = cand.shape
    ids = lax.broadcasted_iota(jnp.int32, (ways, table.shape[1]), 1)
    diagonal = lax.broadcasted_iota(jnp.int32, (ways, ways), 0) == lax.broadcasted_iota(
        jnp.int32, (ways, ways), 1
    )
    top = jnp.max(teacher, axis=1, keepdims=True)
    log_teacher = teacher - top
    log_teacher = log_teacher - jnp.log(jnp.sum(jnp.exp(log_teacher), axis=1, keepdims=True))
    prob = jnp.exp(log_teacher)
    entropy = jnp.sum(prob * log_teacher, axis=1, keepdims=True)
    meta_buf[me] = jnp.zeros(meta_buf.shape[1:], jnp.float32)
    for q in range(count):
        line = cand[q : q + 1, :].astype(jnp.float32)
        column = jnp.sum(jnp.where(diagonal, line, 0.0), axis=1, keepdims=True).astype(jnp.int32)
        row = jnp.sum(jnp.where(column == ids, table, 0.0), axis=1, keepdims=True)
        row = jnp.sum(jnp.where(diagonal, row, 0.0), axis=0, keepdims=True)
        meta_buf[me, q : q + 1, :ways] = row
    meta_buf[me, count : 2 * count, :ways] = prob
    for q in range(count):
        meta_buf[me, 2 * count + q : 2 * count + q + 1, :] = jnp.broadcast_to(
            weights[:, q : q + 1], (1, LANES)
        )
    meta_buf[me, 3 * count : 4 * count, :] = jnp.broadcast_to(entropy, (count, LANES))


def place_candidates(count, ways, meta_ref, hits_ref, mass_ref):
    groups = meta_ref.shape[0]
    spots = lax.broadcasted_iota(jnp.int32, (ways, hits_ref.shape[1]), 1)
    for source in range(groups):
        turned = jnp.transpose(meta_ref[source])
        for q in range(count):
            hot = turned[:ways, q : q + 1].astype(jnp.int32) == spots
            place = source * count + q
            hits_ref[place : place + 1, :] = jnp.sum(
                jnp.where(hot, 1.0, 0.0), axis=0, keepdims=True
            )
            mass_ref[place : place + 1, :] = jnp.sum(
                jnp.where(hot, turned[:ways, count + q : count + q + 1], 0.0),
                axis=0,
                keepdims=True,
            )


def fused_kernel(
    groups, replicas,
    queries_hbm, cand_hbm, map_hbm, teacher_hbm, weights_hbm, lengths_hbm, passages_hbm,
    out_ref, grad_ref, loss_ref,
    raw, doubled, cleared, held, power, inverse, lse, query_buf, folded, meta_buf,
    hits_ref, mass_ref, pick_ref, score_buf, weight_buf, grade_buf, query_weight, query_entropy,
    partial_buf, arrived, loss_buf, cand_ref, map_ref, teacher_ref, weights_ref, lengths_ref,
    load_sem, small_sem, send_sem, recv_sem, wsend_sem, wrecv_sem,
):
    f32, bf16 = jnp.float32, jnp.bfloat16
    me = lax.axis_index("grp")
    mine = lax.axis_index("rep")
    greet(groups, replicas, me, mine)
    tokens, block, dim = raw.shape
    count, ways = cand_ref.shape
    own_rows = query_buf.shape[1]
    width = groups * own_rows
    half = width // 2
    total = groups * count
    rows = held.shape[2]
    blocks = block // rows
    own_copy = pltpu.make_async_copy(queries_hbm, query_buf.at[0], small_sem.at[0])
    own_copy.start()
    loads = []
    pieces = load_sem.shape[0]
    for k in range(pieces):
        at = pl.ds(k * (tokens // pieces), tokens // pieces)
        loads.append(pltpu.make_async_copy(passages_hbm.at[at], raw.at[at], load_sem.at[k]))
    small = []
    for k, (there, here) in enumerate(
        (
            (cand_hbm, cand_ref), (map_hbm, map_ref), (teacher_hbm, teacher_ref),
            (weights_hbm, weights_ref), (lengths_hbm, lengths_ref),
        )
    ):
        small.append(pltpu.make_async_copy(there, here, small_sem.at[1 + k]))
    for copy in small + loads:
        copy.start()

    def exchange(source, target, which, turns):
        copies = {}
        for turn in turns:
            copies[turn] = pltpu.make_async_remote_copy(
                src_ref=source(turn),
                dst_ref=target(turn),
                send_sem=send_sem.at[which, turn],
                recv_sem=recv_sem.at[which, turn],
                device_id={"grp": partner(me, turn)},
                device_id_type=MESH,
            )
            copies[turn].start()
        return copies

    def across(buf, which):
        copies = []
        for step in range(1, replicas):
            copies.append(
                pltpu.make_async_remote_copy(
                    src_ref=buf.at[mine],
                    dst_ref=buf.at[mine],
                    send_sem=wsend_sem.at[which, step],
                    recv_sem=wrecv_sem.at[which, step],
                    device_id={"rep": lax.rem(mine + step, replicas)},
                    device_id_type=MESH,
                )
            )
            copies[-1].start()
        return copies

    near = range(1, groups)
    far = range(groups - 1, 0, -1)
    own_copy.wait()
    greeted(groups, replicas)
    query_copies = exchange(lambda _: query_buf.at[0], lambda t: query_buf.at[t], 0, near)

    for copy in small:
        copy.wait()
    share_meta(
        me, cand_ref[...], map_ref[...].astype(f32), teacher_ref[...], weights_ref[...], meta_buf
    )
    meta_copies = exchange(lambda _: meta_buf.at[me], lambda _: meta_buf.at[me], 1, far)

    wide = jnp.transpose(
        jnp.broadcast_to(lengths_ref[...].astype(f32), (LANES, lengths_ref.shape[1]))
    )
    wide16 = wide.astype(bf16)
    column = lax.broadcasted_iota(jnp.int32, (1, width), 1)
    each = own_rows // count
    turn = column // own_rows
    source = jnp.zeros_like(turn)
    for k in range(groups):
        source = jnp.where(turn == k, partner(me, k), source)
    query = source * count + (column - turn * own_rows) // each
    pick = jnp.where(query == lax.broadcasted_iota(jnp.int32, (total, width), 0), 1.0, 0.0)
    pick_ref[...] = pick
    for copy in loads:
        copy.wait()
    first_token = raw[0]
    prep = span_of(tokens, 12)

    def prepare(k, _):
        for j in range(prep):
            at = k * prep + j
            here = raw[at]
            usable = at.astype(f32).astype(bf16) < wide16
            known = jnp.where(usable, here, first_token)
            doubled[at, :, :dim] = known
            doubled[at, :, dim:] = known
            cleared[at] = jnp.where(usable, here, jnp.zeros_like(here))
        return 0

    lax.fori_loop(0, tokens // prep, prepare, 0)

    bite = span_of(tokens, 4)
    units = [(h, b) for h in range(2) for b in range(blocks)]
    above = None
    for u in range(len(units) + 1):
        if u < len(units):
            h, b = units[u]
            if b == 0:
                span = slice(h * (groups // 2), (h + 1) * (groups // 2))
                for t in range(groups)[span]:
                    if t:
                        query_copies[t].wait()
                scaled = query_buf[span].reshape(half, dim).astype(f32) * to_base2
                upper = scaled.astype(bf16)
                folded[h, :, :dim] = upper
                folded[h, :, dim:] = (scaled - upper.astype(f32)).astype(bf16)
            products = lax.dot_general(
                doubled[:, b * rows : (b + 1) * rows, :].reshape(tokens * rows, 2 * dim),
                folded[h], (((1,), (1,)), ((), ())), preferred_element_type=f32,
            ).reshape(tokens, rows, half)
            highest = None
        if u > 0:
            h0, b0 = units[u - 1]
            summed = jnp.zeros((rows, half), f32)
        for first in range(0, tokens, bite):
            at = slice(first, first + bite)
            if u < len(units):
                held[u % 2, at] = products[at]
                top = jnp.max(products[at], axis=0)
                highest = top if highest is None else jnp.maximum(highest, top)
            if u > 0:
                powers = jnp.exp2(held[(u - 1) % 2, at] - above[None])
                power[h0, b0, at] = powers.astype(bf16)
                summed = summed + jnp.sum(powers, axis=0)
        if u > 0:
            at = slice(b0 * rows, (b0 + 1) * rows)
            to = slice(h0 * half, (h0 + 1) * half)
            unused = (tokens - wide[at, :1]) * jnp.exp2(held[(u - 1) % 2, 0] - above)
            summed = summed - unused
            lse[at, to] = above + jnp.log2(summed)
            inverse[at, to] = 1.0 / summed
        above = highest

    scores = lax.dot_general(
        pick_ref[...], lse[...] * (1.0 / to_base2), (((1,), (1,)), ((), ())),
        precision=HIGH, preferred_element_type=f32,
    )
    score_buf[me, :, :block] = scores[: total // 2]
    score_buf[me, :, block:] = scores[total // 2 :]
    score_copies = exchange(lambda _: score_buf.at[me], lambda _: score_buf.at[me], 2, far)
    for t in meta_copies:
        meta_copies[t].wait()
    for owner in range(groups):
        at = slice(owner * count, (owner + 1) * count)
        query_weight[at, :] = meta_buf[owner, 2 * count : 3 * count, :]
        query_entropy[at, :] = meta_buf[owner, 3 * count : 4 * count, :]
    weight_buf[mine] = jnp.broadcast_to(
        jnp.sum(query_weight[...], axis=0, keepdims=True), weight_buf.shape[1:]
    )
    weight_copies = across(weight_buf, 0)
    place_candidates(count, ways, meta_buf, hits_ref, mass_ref)
    for copy in weight_copies:
        copy.wait()
    weights = query_weight[:, :1]
    weight_sum = jnp.sum(weight_buf[...], axis=0)[:1, :1]
    factor = (total * replicas) * weights / weight_sum
    hits = hits_ref[...]
    mass = mass_ref[...]
    asked = hits > 0.0
    for t in score_copies:
        score_copies[t].wait()
    left = lax.broadcasted_iota(jnp.int32, (total // 2, LANES), 1) < block
    tiles = []
    for owner in range(0, groups, 2):
        one, two = score_buf[owner], score_buf[owner + 1]
        tiles.append(
            jnp.concatenate(
                [
                    jnp.where(left, one, pltpu.roll(two, block, 1)),
                    jnp.where(left, pltpu.roll(one, block, 1), two),
                ],
                axis=0,
            )
        )
    scores = jnp.concatenate(tiles, axis=1)
    masked = jnp.where(asked, scores, -1e30)
    highest = jnp.max(masked, axis=1, keepdims=True)
    summed = jnp.sum(hits * jnp.exp(masked - highest), axis=1, keepdims=True)
    log_student = jnp.where(asked, scores - (highest + jnp.log(summed)), -1e30)
    grade_buf[...] = factor * (hits * jnp.exp(log_student) - mass)
    pair = grade_buf[:, pl.ds(pl.multiple_of(lax.div(me, 2) * LANES, LANES), LANES)]
    odd = jnp.broadcast_to(lax.rem(me, 2), pair.shape) == 1
    own = jnp.where(odd, pltpu.roll(pair, block, 1), pair)[:, :block]
    upper = own.astype(bf16)
    lower = (own - upper.astype(f32)).astype(bf16)
    pick16 = pick_ref[...].astype(bf16)
    spread = lax.dot_general(
        jnp.concatenate([upper, lower], axis=0), jnp.concatenate([pick16, pick16], axis=0),
        (((0,), (0,)), ((), ())), preferred_element_type=f32,
    )
    scale = (inverse[...] * spread).astype(bf16)

    partial_copies = {}
    for h in (1, 0):
        turned = None
        for b in range(blocks):
            part = scale[b * rows : (b + 1) * rows, h * half : (h + 1) * half][None]
            scaled = power[h, b] * part
            power[h, b] = scaled
            piece = lax.dot_general(
                cleared[:, b * rows : (b + 1) * rows, :].reshape(tokens * rows, dim),
                scaled.reshape(tokens * rows, half),
                (((0,), (0,)), ((), ())), preferred_element_type=f32,
            )
            turned = piece if turned is None else turned + piece
        span = slice(h * (groups // 2), (h + 1) * (groups // 2))
        partial_buf[span] = jnp.transpose(turned).astype(bf16).reshape(
            groups // 2, own_rows, dim
        )
        partial_copies.update(
            exchange(
                lambda t: partial_buf.at[t], lambda t: arrived.at[t], 3,
                [t for t in range(groups)[span][::-1] if t],
            )
        )
    crossed = jnp.sum(jnp.where(asked, mass * log_student, 0.0), axis=1, keepdims=True)
    divergence = query_entropy[:, :1] - crossed
    loss_buf[mine] = jnp.broadcast_to(
        jnp.sum(weights * divergence, axis=0, keepdims=True) / weight_sum, loss_buf.shape[1:]
    )
    loss_copies = across(loss_buf, 1)

    for b in range(blocks):
        at = slice(b * rows, (b + 1) * rows)
        token_grad = None
        for h in range(2):
            span = slice(h * (groups // 2), (h + 1) * (groups // 2))
            piece = jnp.dot(
                power[h, b].reshape(tokens * rows, half),
                query_buf[span].reshape(half, dim), preferred_element_type=f32,
            )
            token_grad = piece if token_grad is None else token_grad + piece
        token_grad = token_grad.reshape(tokens, rows, dim)
        for first in range(0, tokens, bite):
            for j in range(first, first + bite):
                usable = jnp.full((), j, bf16) < wide16[at]
                out_ref[j, at, :] = jnp.where(
                    usable, token_grad[j].astype(bf16), jnp.zeros((rows, dim), bf16)
                )

    for t in partial_copies:
        partial_copies[t].wait()
    for copy in loss_copies:
        copy.wait()
    grad_ref[...] = partial_buf[0].astype(f32) + jnp.sum(
        arrived[1:].astype(f32), axis=0
    )
    loss_ref[...] = jnp.sum(loss_buf[...], axis=0)[:1, :1]


def finish_kernel(out_ref, grad_ref, loss_ref, out_hbm, grad_hbm, loss_hbm, sem):
    copies = []
    tokens = out_ref.shape[0]
    pieces = sem.shape[0] - 2
    for k in range(pieces):
        at = pl.ds(k * (tokens // pieces), tokens // pieces)
        copies.append(pltpu.make_async_copy(out_ref.at[at], out_hbm.at[at], sem.at[k]))
    copies.append(pltpu.make_async_copy(grad_ref, grad_hbm, sem.at[pieces]))
    copies.append(pltpu.make_async_copy(loss_ref, loss_hbm, sem.at[pieces + 1]))
    for copy in copies:
        copy.start()
    for copy in copies:
        copy.wait()


def fused(queries, passages, lengths, cand_ids, owner_map, teacher, weights):
    groups = lax.axis_size("grp")
    replicas = lax.axis_size("rep")
    count, _, query_len, dim = queries.shape
    block, _, tokens, _ = passages.shape
    ways = cand_ids.shape[2]
    own_rows = count * query_len
    width = groups * own_rows
    total = groups * count
    rows = 16
    f32, bf16, i32 = jnp.float32, jnp.bfloat16, jnp.int32
    dma = pltpu.SemaphoreType.DMA
    meta_rows = -(-4 * count // 8) * 8
    vmem = pltpu.VMEM
    anywhere = pl.BlockSpec(memory_space=pl.ANY)
    pieces = span_of(tokens, 5)
    results = pl.pallas_call(
        functools.partial(fused_kernel, groups, replicas),
        name="fused",
        out_shape=[
            vmem((tokens, block, dim), bf16),
            vmem((own_rows, dim), f32),
            vmem((1, 1), f32),
        ],
        in_specs=[anywhere] * 7,
        out_specs=[VMEM_SPEC] * 3,
        scratch_shapes=[
            vmem((tokens, block, dim), bf16),
            vmem((tokens, block, 2 * dim), bf16),
            vmem((tokens, block, dim), bf16),
            vmem((2, tokens, rows, width // 2), f32),
            vmem((2, block // rows, tokens, rows, width // 2), bf16),
            vmem((block, width), f32),
            vmem((block, width), f32),
            vmem((groups, own_rows, dim), bf16),
            vmem((2, width // 2, 2 * dim), bf16),
            vmem((groups, meta_rows, LANES), f32),
            vmem((total, groups * block), f32),
            vmem((total, groups * block), f32),
            vmem((total, width), f32),
            vmem((groups, total // 2, LANES), f32),
            vmem((replicas, 8, LANES), f32),
            vmem((total, groups * block), f32),
            vmem((total, LANES), f32),
            vmem((total, LANES), f32),
            vmem((groups, own_rows, dim), bf16),
            vmem((groups, own_rows, dim), bf16),
            vmem((replicas, 8, LANES), f32),
            vmem((count, ways), i32),
            vmem((1, groups * block), i32),
            vmem((count, ways), f32),
            vmem((1, count), f32),
            vmem((1, block), i32),
            dma((pieces,)),
            dma((6,)),
            dma((4, groups)),
            dma((4, groups)),
            dma((2, replicas)),
            dma((2, replicas)),
        ],
        compiler_params=pltpu.CompilerParams(
            collective_id=3, has_side_effects=True, vmem_limit_bytes=FUSED_VMEM
        ),
    )(
        queries.reshape(own_rows, dim),
        cand_ids[:, 0],
        owner_map,
        teacher[:, 0],
        jnp.transpose(weights),
        lengths.reshape(1, block),
        jnp.transpose(passages[:, 0], (1, 0, 2)),
    )
    passage_grad, query_grad, loss = pl.pallas_call(
        finish_kernel,
        name="finish",
        out_shape=[
            jax.ShapeDtypeStruct((tokens, block, dim), bf16),
            jax.ShapeDtypeStruct((own_rows, dim), f32),
            jax.ShapeDtypeStruct((1, 1), f32),
        ],
        in_specs=[VMEM_SPEC] * 3,
        out_specs=[anywhere] * 3,
        scratch_shapes=[dma((pieces + 2,))],
    )(*(pltpu.with_memory_space_constraint(x, pltpu.VMEM) for x in results))
    return (
        loss.reshape(()),
        query_grad.reshape(count, 1, query_len, dim),
        jnp.transpose(passage_grad, (1, 0, 2))[:, None],
    )


FUSED_VMEM = 52 * 2**20


def fits(groups, queries, passages):
    width = groups * queries.shape[0] * queries.shape[2]
    block, _, tokens, dim = passages.shape
    need = tokens * width * (2 * block + 4 * 16) + 10 * tokens * block * dim
    need += 8 * width * (2 * block + 2 * dim)
    whole = groups & (groups - 1) == 0 and groups > 1 and width % (2 * LANES) == 0
    return whole and 2 * block == LANES and dim == LANES and tokens <= 256 and need < FUSED_VMEM


def step(*args):
    if fits(lax.axis_size("grp"), args[0], args[1]):
        return fused(*args)
    return on_device(*args)


def solution(mesh):
    return jax.shard_map(
        step,
        mesh=mesh,
        in_specs=(
            P("grp", "rep", None, None),
            P("grp", "rep", None, None),
            P("grp", "rep"),
            P("grp", "rep", None),
            P("rep", None),
            P("grp", "rep", None),
            P("grp", "rep"),
        ),
        out_specs=(P(), P("grp", "rep", None, None), P("grp", "rep", None, None)),
        check_vma=False,
    )
```

```python
import functools
import math

import jax
import jax.numpy as jnp
from jax import lax
from jax.experimental import pallas as pl
from jax.experimental.pallas import tpu as pltpu
from jax.sharding import PartitionSpec as P

temper = 0.05
to_base2 = 1.0 / (temper * math.log(2.0))
LANES = 128
MESH = pl.DeviceIdType.MESH
HIGH = lax.Precision.HIGHEST
VMEM_SPEC = pl.BlockSpec(memory_space=pltpu.VMEM)


def greet(groups, replicas, me, mine):
    barrier = pltpu.get_barrier_semaphore()
    for step in range(1, groups):
        pl.semaphore_signal(
            barrier, inc=1, device_id={"grp": lax.rem(me + step, groups)}, device_id_type=MESH
        )
    for step in range(1, replicas):
        pl.semaphore_signal(
            barrier, inc=1, device_id={"rep": lax.rem(mine + step, replicas)}, device_id_type=MESH
        )


def greeted(groups, replicas):
    pl.semaphore_wait(pltpu.get_barrier_semaphore(), groups - 1 + replicas - 1)


def share_kernel(
    groups, block, queries_ref, cand_ref, map_ref, teacher_ref, weights_ref,
    all_queries, all_meta, query_buf, meta_buf, send_sem, recv_sem,
):
    me = lax.axis_index("grp")
    greet(groups, 1, me, 0)
    count, ways = cand_ref.shape
    table = map_ref[...].astype(jnp.float32)
    ids = lax.broadcasted_iota(jnp.int32, (ways, table.shape[1]), 1)
    diagonal = lax.broadcasted_iota(jnp.int32, (ways, ways), 0) == lax.broadcasted_iota(
        jnp.int32, (ways, ways), 1
    )
    teacher = teacher_ref[...]
    top = jnp.max(teacher, axis=1, keepdims=True)
    log_teacher = teacher - top
    log_teacher = log_teacher - jnp.log(jnp.sum(jnp.exp(log_teacher), axis=1, keepdims=True))
    prob = jnp.exp(log_teacher)
    entropy = jnp.sum(prob * log_teacher, axis=1, keepdims=True)
    meta_buf[me] = jnp.zeros(meta_buf.shape[1:], jnp.float32)
    for q in range(count):
        line = cand_ref[q : q + 1, :].astype(jnp.float32)
        column = jnp.sum(jnp.where(diagonal, line, 0.0), axis=1, keepdims=True).astype(jnp.int32)
        row = jnp.sum(jnp.where(column == ids, table, 0.0), axis=1, keepdims=True)
        row = jnp.sum(jnp.where(diagonal, row, 0.0), axis=0, keepdims=True)
        meta_buf[me, q : q + 1, :ways] = row
    meta_buf[me, count : 2 * count, :ways] = prob
    for q in range(count):
        meta_buf[me, 2 * count + q : 2 * count + q + 1, :] = jnp.broadcast_to(
            weights_ref[:, q : q + 1], (1, LANES)
        )
    meta_buf[me, 3 * count : 4 * count, :] = jnp.broadcast_to(entropy, (count, LANES))
    query_buf[me] = queries_ref[...]
    greeted(groups, 1)
    copies = []
    for step in range(1, groups):
        peer = lax.rem(me + step, groups)
        for which, buf in enumerate((query_buf, meta_buf)):
            copies.append(
                pltpu.make_async_remote_copy(
                    src_ref=buf.at[me],
                    dst_ref=buf.at[me],
                    send_sem=send_sem.at[which, step],
                    recv_sem=recv_sem.at[which, step],
                    device_id={"grp": peer},
                    device_id_type=MESH,
                )
            )
            copies[-1].start()
    for copy in copies:
        copy.wait()
    all_queries[...] = query_buf[...]
    all_meta[...] = meta_buf[...]


def span_of(tokens, limit):
    return max(size for size in range(1, limit + 1) if tokens % size == 0)


def lengths_of(lengths_ref, first, rows, width):
    index = lax.broadcasted_iota(jnp.int32, (rows, width), 0)
    found = jnp.zeros((rows, width), jnp.int32)
    for k in range(rows):
        found = jnp.where(index == k, lengths_ref[first + k], found)
    return found


def forward_kernel(
    count, ways, block, lengths_ref, passages_ref, queries_ref, meta_ref,
    lse_ref, score_ref, hits_ref, mass_ref, held, all_lse,
):
    step = pl.program_id(0)
    part = pl.program_id(1)
    groups = meta_ref.shape[0]
    tokens, rows, dim = passages_ref.shape
    width = queries_ref.shape[0]
    slot = score_ref.shape[1]

    @pl.when((step == 0) & (part == 0))
    def _():
        spots = lax.broadcasted_iota(jnp.int32, (ways, groups * slot), 1)
        for source in range(groups):
            turned = jnp.transpose(meta_ref[source])
            for q in range(count):
                row = turned[:ways, q : q + 1].astype(jnp.int32)
                spot = row + (slot - block) * (row // block)
                hot = spot == spots
                place = source * count + q
                hits_ref[place : place + 1, :] = jnp.sum(
                    jnp.where(hot, 1.0, 0.0), axis=0, keepdims=True
                )
                mass_ref[place : place + 1, :] = jnp.sum(
                    jnp.where(hot, turned[:ways, count + q : count + q + 1], 0.0),
                    axis=0,
                    keepdims=True,
                )

    lengths = lengths_of(lengths_ref, step * rows, rows, width)
    size = span_of(tokens, 20)
    highest = jnp.full((rows, width), -1e30, jnp.float32)
    for first in range(0, tokens, size):
        products = lax.dot_general(
            passages_ref[first : first + size].reshape(size * rows, dim), queries_ref[...],
            (((1,), (1,)), ((), ())), preferred_element_type=jnp.float32,
        )
        for j in range(size):
            scaled = jnp.where(
                first + j < lengths, products[j * rows : (j + 1) * rows] * to_base2, -1e30
            )
            held[first + j] = scaled
            highest = jnp.maximum(highest, scaled)
    summed = jnp.zeros((rows, width), jnp.float32)
    for j in range(tokens):
        summed = summed + jnp.exp2(held[j] - highest)
    lse = highest + jnp.log2(summed)
    lse_ref[...] = lse
    all_lse[step, part] = lse

    @pl.when((step == pl.num_programs(0) - 1) & (part == pl.num_programs(1) - 1))
    def _():
        total = score_ref.shape[0]
        parts = all_lse.shape[1]
        each = width * parts // total
        score_ref[...] = jnp.zeros_like(score_ref)
        belongs = lax.broadcasted_iota(jnp.int32, (total // parts, width), 1) // each
        pick = jnp.where(
            belongs == lax.broadcasted_iota(jnp.int32, (total // parts, width), 0), 1.0, 0.0
        )
        span = total // parts
        for k in range(parts):
            matched = jnp.concatenate(
                [all_lse[i, k] for i in range(all_lse.shape[0])], axis=0
            ) * (1.0 / to_base2)
            score_ref[k * span : (k + 1) * span, :block] = lax.dot_general(
                pick, matched, (((1,), (1,)), ((), ())),
                precision=HIGH, preferred_element_type=jnp.float32,
            )


def grade_kernel(
    groups, replicas, score_ref, hits_ref, mass_ref, meta_ref, grad_ref, loss_ref,
    score_buf, weight_buf, grad_buf, query_weight, query_entropy,
    send_sem, recv_sem, wsend_sem, wrecv_sem,
):
    me = lax.axis_index("grp")
    mine = lax.axis_index("rep")
    greet(groups, replicas, me, mine)
    total, slot = score_ref.shape
    count = total // groups
    for source in range(groups):
        span = slice(source * count, (source + 1) * count)
        query_weight[span, :] = meta_ref[source, 2 * count : 3 * count, :]
        query_entropy[span, :] = meta_ref[source, 3 * count : 4 * count, :]
    weights = query_weight[:, :1]
    score_buf[me] = score_ref[...]
    weight_buf[mine] = jnp.broadcast_to(
        jnp.sum(query_weight[...], axis=0, keepdims=True), weight_buf.shape[1:]
    )
    greeted(groups, replicas)
    copies = []
    for step in range(1, groups):
        copies.append(
            pltpu.make_async_remote_copy(
                src_ref=score_buf.at[me],
                dst_ref=score_buf.at[me],
                send_sem=send_sem.at[step],
                recv_sem=recv_sem.at[step],
                device_id={"grp": lax.rem(me + step, groups)},
                device_id_type=MESH,
            )
        )
        copies[-1].start()
    for step in range(1, replicas):
        copies.append(
            pltpu.make_async_remote_copy(
                src_ref=weight_buf.at[mine],
                dst_ref=weight_buf.at[mine],
                send_sem=wsend_sem.at[step],
                recv_sem=wrecv_sem.at[step],
                device_id={"rep": lax.rem(mine + step, replicas)},
                device_id_type=MESH,
            )
        )
        copies[-1].start()
    for copy in copies:
        copy.wait()
    weight_sum = jnp.sum(weight_buf[...], axis=0)[:1, :1]
    scores = jnp.concatenate([score_buf[owner] for owner in range(groups)], axis=1)
    hits = hits_ref[...]
    mass = mass_ref[...]
    asked = hits > 0.0
    held = jnp.where(asked, scores, -1e30)
    highest = jnp.max(held, axis=1, keepdims=True)
    summed = jnp.sum(hits * jnp.exp(held - highest), axis=1, keepdims=True)
    log_student = jnp.where(asked, scores - (highest + jnp.log(summed)), -1e30)
    student = hits * jnp.exp(log_student)
    crossed = jnp.sum(jnp.where(asked, mass * log_student, 0.0), axis=1, keepdims=True)
    divergence = query_entropy[:, :1] - crossed
    grad_buf[...] = (total * replicas) * weights / weight_sum * (student - mass)
    own = grad_buf[:, pl.ds(pl.multiple_of(me * slot, slot), slot)]
    width = grad_ref.shape[1]
    each = width // total
    belongs = lax.broadcasted_iota(jnp.int32, (total, width), 1) // each
    pick = jnp.where(belongs == lax.broadcasted_iota(jnp.int32, (total, width), 0), 1.0, 0.0)
    spread = lax.dot_general(
        own, pick, (((0,), (0,)), ((), ())), precision=HIGH, preferred_element_type=jnp.float32
    )
    grad_ref[...] = spread[: grad_ref.shape[0]]
    loss_ref[...] = jnp.broadcast_to(
        jnp.sum(weights * divergence, axis=0, keepdims=True) / weight_sum, loss_ref.shape
    )


def backward_kernel(
    lengths_ref, passages_ref, queries_ref, lse_ref, grad_ref, out_ref, partial_ref,
    total, token_total,
):
    step = pl.program_id(0)
    part = pl.program_id(1)
    parts = total.shape[0]
    tokens, rows, dim = passages_ref.shape
    width = queries_ref.shape[0]

    @pl.when(step == 0)
    def _():
        total[part] = jnp.zeros(total.shape[1:], jnp.float32)

    if parts > 1:

        @pl.when(part == 0)
        def _():
            token_total[...] = jnp.zeros_like(token_total)

    lengths = lengths_of(lengths_ref, step * rows, rows, width)[None]
    lse = lse_ref[...][None]
    grad = grad_ref[...][None]
    queries = queries_ref[...]
    size = span_of(tokens, 36)
    added = None
    for first in range(0, tokens, size):
        passage = passages_ref[first : first + size].reshape(size * rows, dim)
        products = lax.dot_general(
            passage, queries, (((1,), (1,)), ((), ())), preferred_element_type=jnp.float32
        ).reshape(size, rows, width)
        position = first + lax.broadcasted_iota(jnp.int32, (size, 1, 1), 0)
        powers = jnp.exp2(jnp.where(position < lengths, products * to_base2 - lse, -1e30))
        scaled_grad = (powers * grad).astype(jnp.bfloat16).reshape(size * rows, width)
        token_grad = jnp.dot(scaled_grad, queries, preferred_element_type=jnp.float32).reshape(
            size, rows, dim
        )
        if parts > 1:
            token_total[first : first + size] += token_grad
        else:
            out_ref[first : first + size] = token_grad.astype(jnp.bfloat16)
        piece = lax.dot_general(
            passage, scaled_grad, (((0,), (0,)), ((), ())), preferred_element_type=jnp.float32
        )
        added = piece if added is None else added + piece
    total[part] += added

    if parts > 1:

        @pl.when(part == parts - 1)
        def _():
            out_ref[...] = token_total[...].astype(jnp.bfloat16)

    @pl.when(step == pl.num_programs(0) - 1)
    def _():
        partial_ref[pl.ds(pl.multiple_of(part * width, width), width), :] = jnp.transpose(
            total[part]
        ).astype(partial_ref.dtype)


def collect_kernel(
    groups, replicas, partial_ref, loss_ref, grad_ref, loss_out,
    arrived, loss_buf, send_sem, recv_sem, lsend_sem, lrecv_sem,
):
    me = lax.axis_index("grp")
    mine = lax.axis_index("rep")
    greet(groups, replicas, me, mine)
    loss_buf[mine] = loss_ref[...]
    greeted(groups, replicas)
    copies = []
    for step in range(1, groups):
        peer = lax.rem(me + step, groups)
        copies.append(
            pltpu.make_async_remote_copy(
                src_ref=partial_ref.at[peer],
                dst_ref=arrived.at[me],
                send_sem=send_sem.at[step],
                recv_sem=recv_sem.at[step],
                device_id={"grp": peer},
                device_id_type=MESH,
            )
        )
        copies[-1].start()
    for step in range(1, replicas):
        copies.append(
            pltpu.make_async_remote_copy(
                src_ref=loss_buf.at[mine],
                dst_ref=loss_buf.at[mine],
                send_sem=lsend_sem.at[step],
                recv_sem=lrecv_sem.at[step],
                device_id={"rep": lax.rem(mine + step, replicas)},
                device_id_type=MESH,
            )
        )
        copies[-1].start()
    arrived[me] = partial_ref[me]
    for copy in copies:
        copy.wait()
    grad_ref[...] = jnp.sum(arrived[...].astype(jnp.float32), axis=0)
    loss_out[...] = jnp.sum(loss_buf[...], axis=0)[:1, :1]


def on_device(queries, passages, lengths, cand_ids, owner_map, teacher, weights):
    groups = lax.axis_size("grp")
    replicas = lax.axis_size("rep")
    count, _, query_len, dim = queries.shape
    block, _, tokens, _ = passages.shape
    ways = cand_ids.shape[2]
    own_rows = count * query_len
    width = groups * own_rows
    total = groups * count
    slot = -(-block // LANES) * LANES
    f32 = jnp.float32
    dma = pltpu.SemaphoreType.DMA
    meta_rows = -(-4 * count // 8) * 8
    all_queries, all_meta = pl.pallas_call(
        functools.partial(share_kernel, groups, block),
        name="share",
        out_shape=[
            jax.ShapeDtypeStruct((groups, own_rows, dim), queries.dtype),
            jax.ShapeDtypeStruct((groups, meta_rows, LANES), f32),
        ],
        in_specs=[VMEM_SPEC] * 5,
        out_specs=[VMEM_SPEC] * 2,
        scratch_shapes=[
            pltpu.VMEM((groups, own_rows, dim), queries.dtype),
            pltpu.VMEM((groups, meta_rows, LANES), f32),
            dma((2, groups)),
            dma((2, groups)),
        ],
        compiler_params=pltpu.CompilerParams(collective_id=0, has_side_effects=True),
    )(
        queries.reshape(own_rows, dim),
        cand_ids[:, 0],
        owner_map,
        teacher[:, 0],
        jnp.transpose(weights),
    )
    flat_queries = all_queries.reshape(width, dim)
    flat_passages = jnp.transpose(passages[:, 0], (1, 0, 2))
    flat_lengths = lengths.reshape(block)
    rows = 16 if block % 16 == 0 else block
    chunk = width if width <= 512 else width // (width // 512)
    parts = width // chunk
    grid = (block // rows, parts)
    whole = lambda *shape: pl.BlockSpec(shape, lambda i, k, *_: (0,) * len(shape))
    passage_spec = pl.BlockSpec((tokens, rows, dim), lambda i, k, *_: (0, i, 0))
    query_spec = pl.BlockSpec((chunk, dim), lambda i, k, *_: (k, 0))
    row_spec = pl.BlockSpec((rows, chunk), lambda i, k, *_: (i, k))
    both = pltpu.CompilerParams(dimension_semantics=("arbitrary", "arbitrary"))
    lse, score, hits, mass = pl.pallas_call(
        functools.partial(forward_kernel, count, ways, block),
        name="forward",
        grid_spec=pltpu.PrefetchScalarGridSpec(
            num_scalar_prefetch=1,
            grid=grid,
            in_specs=[passage_spec, query_spec, whole(groups, meta_rows, LANES)],
            out_specs=[
                row_spec,
                whole(total, slot),
                whole(total, groups * slot),
                whole(total, groups * slot),
            ],
            scratch_shapes=[
                pltpu.VMEM((tokens, rows, chunk), f32),
                pltpu.VMEM((*grid, rows, chunk), f32),
            ],
        ),
        out_shape=[
            jax.ShapeDtypeStruct((block, width), f32),
            jax.ShapeDtypeStruct((total, slot), f32),
            jax.ShapeDtypeStruct((total, groups * slot), f32),
            jax.ShapeDtypeStruct((total, groups * slot), f32),
        ],
        compiler_params=both,
    )(flat_lengths, flat_passages, flat_queries, all_meta)
    grad, loss_part = pl.pallas_call(
        functools.partial(grade_kernel, groups, replicas),
        name="grade",
        out_shape=[
            jax.ShapeDtypeStruct((block, width), f32),
            jax.ShapeDtypeStruct((8, LANES), f32),
        ],
        in_specs=[VMEM_SPEC] * 4,
        out_specs=[VMEM_SPEC] * 2,
        scratch_shapes=[
            pltpu.VMEM((groups, total, slot), f32),
            pltpu.VMEM((replicas, 8, LANES), f32),
            pltpu.VMEM((total, groups * slot), f32),
            pltpu.VMEM((total, LANES), f32),
            pltpu.VMEM((total, LANES), f32),
            dma((groups,)),
            dma((groups,)),
            dma((replicas,)),
            dma((replicas,)),
        ],
        compiler_params=pltpu.CompilerParams(collective_id=1, has_side_effects=True),
    )(score, hits, mass, all_meta)
    passage_grad, partial = pl.pallas_call(
        backward_kernel,
        name="backward",
        grid_spec=pltpu.PrefetchScalarGridSpec(
            num_scalar_prefetch=1,
            grid=grid,
            in_specs=[passage_spec, query_spec, row_spec, row_spec],
            out_specs=[passage_spec, whole(width, dim)],
            scratch_shapes=[
                pltpu.VMEM((parts, dim, chunk), f32),
                pltpu.VMEM((tokens, rows, dim) if parts > 1 else (8, rows, dim), f32),
            ],
        ),
        out_shape=[
            jax.ShapeDtypeStruct((tokens, block, dim), jnp.bfloat16),
            jax.ShapeDtypeStruct((width, dim), jnp.bfloat16),
        ],
        compiler_params=both,
    )(flat_lengths, flat_passages, flat_queries, lse, grad)
    query_grad, loss = pl.pallas_call(
        functools.partial(collect_kernel, groups, replicas),
        name="collect",
        out_shape=[
            jax.ShapeDtypeStruct((own_rows, dim), f32),
            jax.ShapeDtypeStruct((1, 1), f32),
        ],
        in_specs=[VMEM_SPEC] * 2,
        out_specs=[VMEM_SPEC] * 2,
        scratch_shapes=[
            pltpu.VMEM((groups, own_rows, dim), jnp.bfloat16),
            pltpu.VMEM((replicas, 8, LANES), f32),
            dma((groups,)),
            dma((groups,)),
            dma((replicas,)),
            dma((replicas,)),
        ],
        compiler_params=pltpu.CompilerParams(collective_id=2, has_side_effects=True),
    )(partial.reshape(groups, own_rows, dim), loss_part)
    return (
        loss.reshape(()),
        query_grad.reshape(count, 1, query_len, dim),
        jnp.transpose(passage_grad, (1, 0, 2))[:, None],
    )


def partner(me, turn):
    peer = me
    bit = 1
    while bit <= turn:
        if turn & bit:
            peer = peer + bit * (1 - 2 * lax.rem(lax.div(me, bit), 2))
        bit *= 2
    return peer


def share_meta(me, cand, table, teacher, weights, meta_buf):
    count, ways = cand.shape
    ids = lax.broadcasted_iota(jnp.int32, (ways, table.shape[1]), 1)
    diagonal = lax.broadcasted_iota(jnp.int32, (ways, ways), 0) == lax.broadcasted_iota(
        jnp.int32, (ways, ways), 1
    )
    top = jnp.max(teacher, axis=1, keepdims=True)
    log_teacher = teacher - top
    log_teacher = log_teacher - jnp.log(jnp.sum(jnp.exp(log_teacher), axis=1, keepdims=True))
    prob = jnp.exp(log_teacher)
    entropy = jnp.sum(prob * log_teacher, axis=1, keepdims=True)
    meta_buf[me] = jnp.zeros(meta_buf.shape[1:], jnp.float32)
    for q in range(count):
        line = cand[q : q + 1, :].astype(jnp.float32)
        column = jnp.sum(jnp.where(diagonal, line, 0.0), axis=1, keepdims=True).astype(jnp.int32)
        row = jnp.sum(jnp.where(column == ids, table, 0.0), axis=1, keepdims=True)
        row = jnp.sum(jnp.where(diagonal, row, 0.0), axis=0, keepdims=True)
        meta_buf[me, q : q + 1, :ways] = row
    meta_buf[me, count : 2 * count, :ways] = prob
    for q in range(count):
        meta_buf[me, 2 * count + q : 2 * count + q + 1, :] = jnp.broadcast_to(
            weights[:, q : q + 1], (1, LANES)
        )
    meta_buf[me, 3 * count : 4 * count, :] = jnp.broadcast_to(entropy, (count, LANES))


def place_candidates(count, ways, meta_ref, hits_ref, mass_ref):
    groups = meta_ref.shape[0]
    spots = lax.broadcasted_iota(jnp.int32, (ways, hits_ref.shape[1]), 1)
    for source in range(groups):
        turned = jnp.transpose(meta_ref[source])
        for q in range(count):
            hot = turned[:ways, q : q + 1].astype(jnp.int32) == spots
            place = source * count + q
            hits_ref[place : place + 1, :] = jnp.sum(
                jnp.where(hot, 1.0, 0.0), axis=0, keepdims=True
            )
            mass_ref[place : place + 1, :] = jnp.sum(
                jnp.where(hot, turned[:ways, count + q : count + q + 1], 0.0),
                axis=0,
                keepdims=True,
            )


def fused_kernel(
    groups, replicas,
    queries_hbm, cand_hbm, map_hbm, teacher_hbm, weights_hbm, lengths_hbm, passages_hbm,
    out_ref, grad_ref,
    raw, doubled, cleared, turned_ref, tops, scales, limits, held, power, inverse, lse, query_buf, folded, meta_buf,
    hits_ref, mass_ref, pick_ref, score_buf, weight_buf, grade_buf, query_weight, query_entropy,
    partial_buf, arrived, loss_buf, cand_ref, map_ref, teacher_ref, weights_ref, lengths_ref,
    load_sem, small_sem, send_sem, recv_sem, wsend_sem, wrecv_sem,
):
    f32, bf16 = jnp.float32, jnp.bfloat16
    me = lax.axis_index("grp")
    mine = lax.axis_index("rep")
    greet(groups, replicas, me, mine)
    tokens, block, dim = raw.shape
    count, ways = cand_ref.shape
    own_rows = query_buf.shape[1]
    width = groups * own_rows
    half = width // 2
    total = groups * count
    rows = held.shape[2]
    blocks = block // rows
    own_copy = pltpu.make_async_copy(queries_hbm, query_buf.at[0], small_sem.at[0])
    own_copy.start()
    loads = []
    pieces = load_sem.shape[0]
    for k in range(pieces):
        at = pl.ds(k * (tokens // pieces), tokens // pieces)
        loads.append(pltpu.make_async_copy(passages_hbm.at[at], raw.at[at], load_sem.at[k]))
    small = []
    for k, (there, here) in enumerate(
        (
            (cand_hbm, cand_ref), (map_hbm, map_ref), (teacher_hbm, teacher_ref),
            (weights_hbm, weights_ref), (lengths_hbm, lengths_ref),
        )
    ):
        small.append(pltpu.make_async_copy(there, here, small_sem.at[1 + k]))
    for copy in small + loads:
        copy.start()

    def exchange(source, target, which, turns):
        copies = {}
        for turn in turns:
            copies[turn] = pltpu.make_async_remote_copy(
                src_ref=source(turn),
                dst_ref=target(turn),
                send_sem=send_sem.at[which, turn],
                recv_sem=recv_sem.at[which, turn],
                device_id={"grp": partner(me, turn)},
                device_id_type=MESH,
            )
            copies[turn].start()
        return copies

    def across(buf, which):
        copies = []
        for step in range(1, replicas):
            copies.append(
                pltpu.make_async_remote_copy(
                    src_ref=buf.at[mine],
                    dst_ref=buf.at[mine],
                    send_sem=wsend_sem.at[which, step],
                    recv_sem=wrecv_sem.at[which, step],
                    device_id={"rep": lax.rem(mine + step, replicas)},
                    device_id_type=MESH,
                )
            )
            copies[-1].start()
        return copies

    near = range(1, groups)
    far = range(groups - 1, 0, -1)
    own_copy.wait()
    greeted(groups, replicas)
    query_copies = exchange(lambda _: query_buf.at[0], lambda t: query_buf.at[t], 0, near)

    for copy in small:
        copy.wait()
    share_meta(
        me, cand_ref[...], map_ref[...].astype(f32), teacher_ref[...], weights_ref[...], meta_buf
    )
    meta_copies = exchange(lambda _: meta_buf.at[me], lambda _: meta_buf.at[me], 1, far)

    wide = jnp.transpose(
        jnp.broadcast_to(lengths_ref[...].astype(f32), (LANES, lengths_ref.shape[1]))
    )
    wide16 = wide.astype(bf16)
    column = lax.broadcasted_iota(jnp.int32, (1, width), 1)
    each = own_rows // count
    turn = column // own_rows
    source = jnp.zeros_like(turn)
    for k in range(groups):
        source = jnp.where(turn == k, partner(me, k), source)
    query = source * count + (column - turn * own_rows) // each
    pick = jnp.where(query == lax.broadcasted_iota(jnp.int32, (total, width), 0), 1.0, 0.0)
    pick_ref[...] = pick
    for copy in loads:
        copy.wait()
    first_token = raw[0]
    prep = span_of(tokens, 12)

    def prepare(k, _):
        for j in range(prep):
            at = k * prep + j
            here = raw[at]
            usable = at.astype(f32).astype(bf16) < wide16
            known = jnp.where(usable, here, first_token)
            doubled[:, at] = known.reshape(blocks, rows, dim)
            cleared[:, at] = jnp.where(usable, here, jnp.zeros_like(here)).reshape(
                blocks, rows, dim
            )
        return 0

    lax.fori_loop(0, tokens // prep, prepare, 0)

    single = jnp.minimum(me + 1, 1)
    bite = span_of(tokens, 180)
    units = [(h, b) for h in range(2) for b in range(blocks)]

    def forward(u):
        ahead = units[u] if u < len(units) else None
        behind = units[u - 1] if u > 0 else None
        highest = None
        if ahead is not None:
            h, b = ahead
            left = doubled[b].reshape(tokens * rows, dim)
            products = lax.dot_general(
                jnp.concatenate([left, left], axis=1), folded[h],
                (((1,), (1,)), ((), ())), preferred_element_type=f32,
            ).reshape(tokens, rows, half)
        if behind is not None:
            h0, b0 = behind
            above = tops[(u - 1) % 2]
            sums = [None] * 2
        peaks = [None] * 2
        for first in range(tokens // 2):
            for line in range(2):
                j = line * (tokens // 2) + first
                if ahead is not None:
                    held[u % 2, j] = products[j]
                    peaks[line] = products[j] if first == 0 else jnp.maximum(peaks[line], products[j])
                if behind is not None:
                    powers = jnp.exp2(held[(u - 1) % 2, j] - above)
                    power[h0, b0, j] = powers.astype(bf16)
                    sums[line] = powers if first == 0 else sums[line] + powers
        if ahead is not None:
            highest = functools.reduce(jnp.maximum, peaks)
        if behind is not None:
            summed = functools.reduce(jnp.add, sums)
        if ahead is not None:
            tops[u % 2] = highest
        if behind is not None:
            at = slice(b0 * rows, (b0 + 1) * rows)
            to = slice(h0 * half, (h0 + 1) * half)
            unused = (tokens - limits[at, :1]) * jnp.exp2(held[(u - 1) % 2, 0] - above)
            summed = summed - unused
            lse[at, to] = above + jnp.log2(summed)
            inverse[at, to] = 1.0 / summed

    limits[...] = wide
    for u in range(len(units) + 1):
        if u < len(units) and units[u][1] == 0:
            h = units[u][0]
            span = slice(h * (groups // 2), (h + 1) * (groups // 2))
            for t in range(groups)[span]:
                if t:
                    query_copies[t].wait()
            scaled = query_buf[span].reshape(half, dim).astype(f32) * to_base2
            upper = scaled.astype(bf16)
            folded[h, :, :dim] = upper
            folded[h, :, dim:] = (scaled - upper.astype(f32)).astype(bf16)

        def trip(_, carry, u=u):
            forward(u)
            return carry

        lax.fori_loop(0, single, trip, 0)

    scores = lax.dot_general(
        pick_ref[...], lse[...] * (1.0 / to_base2), (((1,), (1,)), ((), ())),
        precision=HIGH, preferred_element_type=f32,
    )
    score_buf[me, :, :block] = scores[: total // 2]
    score_buf[me, :, block:] = scores[total // 2 :]
    score_copies = exchange(lambda _: score_buf.at[me], lambda _: score_buf.at[me], 2, far)
    for t in meta_copies:
        meta_copies[t].wait()
    for owner in range(groups):
        at = slice(owner * count, (owner + 1) * count)
        query_weight[at, :] = meta_buf[owner, 2 * count : 3 * count, :]
        query_entropy[at, :] = meta_buf[owner, 3 * count : 4 * count, :]
    weight_buf[mine] = jnp.broadcast_to(
        jnp.sum(query_weight[...], axis=0, keepdims=True), weight_buf.shape[1:]
    )
    weight_copies = across(weight_buf, 0)
    place_candidates(count, ways, meta_buf, hits_ref, mass_ref)
    for b in range(blocks):
        turned_ref[b] = jnp.transpose(cleared[b].reshape(tokens * rows, dim))
    for copy in weight_copies:
        copy.wait()
    weights = query_weight[:, :1]
    weight_sum = jnp.sum(weight_buf[...], axis=0)[:1, :1]
    factor = (total * replicas) * weights / weight_sum
    hits = hits_ref[...]
    mass = mass_ref[...]
    asked = hits > 0.0
    for t in score_copies:
        score_copies[t].wait()
    left = lax.broadcasted_iota(jnp.int32, (total // 2, LANES), 1) < block
    tiles = []
    for owner in range(0, groups, 2):
        one, two = score_buf[owner], score_buf[owner + 1]
        tiles.append(
            jnp.concatenate(
                [
                    jnp.where(left, one, pltpu.roll(two, block, 1)),
                    jnp.where(left, pltpu.roll(one, block, 1), two),
                ],
                axis=0,
            )
        )
    scores = jnp.concatenate(tiles, axis=1)
    masked = jnp.where(asked, scores, -1e30)
    highest = jnp.max(masked, axis=1, keepdims=True)
    summed = jnp.sum(hits * jnp.exp(masked - highest), axis=1, keepdims=True)
    log_student = jnp.where(asked, scores - (highest + jnp.log(summed)), -1e30)
    grade_buf[...] = factor * (hits * jnp.exp(log_student) - mass)
    pair = grade_buf[:, pl.ds(pl.multiple_of(lax.div(me, 2) * LANES, LANES), LANES)]
    odd = jnp.broadcast_to(lax.rem(me, 2), pair.shape) == 1
    own = jnp.where(odd, pltpu.roll(pair, block, 1), pair)[:, :block]
    upper = own.astype(bf16)
    lower = (own - upper.astype(f32)).astype(bf16)
    pick16 = pick_ref[...].astype(bf16)
    spread = lax.dot_general(
        jnp.concatenate([upper, lower], axis=0), jnp.concatenate([pick16, pick16], axis=0),
        (((0,), (0,)), ((), ())), preferred_element_type=f32,
    )
    scale = (inverse[...] * spread).astype(bf16)
    for h in range(2):
        for b in range(blocks):
            scales[h, b] = scale[b * rows : (b + 1) * rows, h * half : (h + 1) * half]

    partial_copies = {}
    for h in (1, 0):

        def backward(_, carry, h=h):
            added = None
            for b in range(blocks):
                piece = jnp.dot(
                    turned_ref[b],
                    (power[h, b] * scales[h, b][None]).reshape(tokens * rows, half),
                    preferred_element_type=f32,
                )
                added = piece if added is None else added + piece
            partial_buf[h * (groups // 2) : (h + 1) * (groups // 2)] = (
                jnp.transpose(added).astype(bf16).reshape(groups // 2, own_rows, dim)
            )
            return carry

        lax.fori_loop(0, single, backward, 0)
        span = slice(h * (groups // 2), (h + 1) * (groups // 2))
        partial_copies.update(
            exchange(
                lambda t: partial_buf.at[t], lambda t: arrived.at[t], 3,
                [t for t in range(groups)[span][::-1] if t],
            )
        )
    crossed = jnp.sum(jnp.where(asked, mass * log_student, 0.0), axis=1, keepdims=True)
    divergence = query_entropy[:, :1] - crossed
    loss_buf[mine] = jnp.broadcast_to(
        jnp.sum(weights * divergence, axis=0, keepdims=True) / weight_sum, loss_buf.shape[1:]
    )
    loss_copies = across(loss_buf, 1)

    def tokenwise(_, carry):
        for b in range(blocks):
            at = slice(b * rows, (b + 1) * rows)
            token_grad = None
            for h in range(2):
                span = slice(h * (groups // 2), (h + 1) * (groups // 2))
                piece = jnp.dot(
                    (power[h, b] * scales[h, b][None]).reshape(tokens * rows, half),
                    query_buf[span].reshape(half, dim), preferred_element_type=f32,
                )
                token_grad = piece if token_grad is None else token_grad + piece
            token_grad = token_grad.reshape(tokens, rows, dim)
            limit = limits[at].astype(bf16)
            for j in range(tokens):
                usable = jnp.full((), j, bf16) < limit
                out_ref[j, at, :] = jnp.where(
                    usable, token_grad[j].astype(bf16), jnp.zeros((rows, dim), bf16)
                )
        return carry

    lax.fori_loop(0, single, tokenwise, 0)

    for t in partial_copies:
        partial_copies[t].wait()
    for copy in loss_copies:
        copy.wait()
    grad_ref[:own_rows, :] = partial_buf[0].astype(f32) + jnp.sum(
        arrived[1:].astype(f32), axis=0
    )
    grad_ref[own_rows:, :] = jnp.sum(loss_buf[...], axis=0)


def finish_kernel(out_ref, grad_ref, out_hbm, grad_hbm, loss_hbm, loss_ref, sem):
    copies = []
    tokens = out_ref.shape[0]
    pieces = sem.shape[0] - 2
    for k in range(pieces):
        at = pl.ds(k * (tokens // pieces), tokens // pieces)
        copies.append(pltpu.make_async_copy(out_ref.at[at], out_hbm.at[at], sem.at[k]))
        copies[-1].start()
    own = grad_hbm.shape[0]
    copies.append(pltpu.make_async_copy(grad_ref.at[pl.ds(0, own)], grad_hbm, sem.at[pieces]))
    copies[-1].start()
    loss_ref[...] = grad_ref[own : own + 1, :1]
    copies.append(pltpu.make_async_copy(loss_ref, loss_hbm, sem.at[pieces + 1]))
    copies[-1].start()
    for copy in copies:
        copy.wait()


def fused(queries, passages, lengths, cand_ids, owner_map, teacher, weights):
    groups = lax.axis_size("grp")
    replicas = lax.axis_size("rep")
    count, _, query_len, dim = queries.shape
    block, _, tokens, _ = passages.shape
    ways = cand_ids.shape[2]
    own_rows = count * query_len
    width = groups * own_rows
    total = groups * count
    rows = 16
    f32, bf16, i32 = jnp.float32, jnp.bfloat16, jnp.int32
    dma = pltpu.SemaphoreType.DMA
    meta_rows = -(-4 * count // 8) * 8
    vmem = pltpu.VMEM
    anywhere = pl.BlockSpec(memory_space=pl.ANY)
    pieces = span_of(tokens, 5)
    results = pl.pallas_call(
        functools.partial(fused_kernel, groups, replicas),
        name="fused",
        out_shape=[
            vmem((tokens, block, dim), bf16),
            vmem((own_rows + 8, dim), f32),
        ],
        in_specs=[anywhere] * 7,
        out_specs=[VMEM_SPEC] * 2,
        scratch_shapes=[
            vmem((tokens, block, dim), bf16),
            vmem((block // rows, tokens, rows, dim), bf16),
            vmem((block // rows, tokens, rows, dim), bf16),
            vmem((block // rows, dim, tokens * rows), bf16),
            vmem((2, rows, width // 2), f32),
            vmem((2, block // rows, rows, width // 2), bf16),
            vmem((block, LANES), f32),
            vmem((2, tokens, rows, width // 2), f32),
            vmem((2, block // rows, tokens, rows, width // 2), bf16),
            vmem((block, width), f32),
            vmem((block, width), f32),
            vmem((groups, own_rows, dim), bf16),
            vmem((2, width // 2, 2 * dim), bf16),
            vmem((groups, meta_rows, LANES), f32),
            vmem((total, groups * block), f32),
            vmem((total, groups * block), f32),
            vmem((total, width), f32),
            vmem((groups, total // 2, LANES), f32),
            vmem((replicas, 8, LANES), f32),
            vmem((total, groups * block), f32),
            vmem((total, LANES), f32),
            vmem((total, LANES), f32),
            vmem((groups, own_rows, dim), bf16),
            vmem((groups, own_rows, dim), bf16),
            vmem((replicas, 8, LANES), f32),
            vmem((count, ways), i32),
            vmem((1, groups * block), i32),
            vmem((count, ways), f32),
            vmem((1, count), f32),
            vmem((1, block), i32),
            dma((pieces,)),
            dma((6,)),
            dma((4, groups)),
            dma((4, groups)),
            dma((2, replicas)),
            dma((2, replicas)),
        ],
        compiler_params=pltpu.CompilerParams(
            collective_id=3, has_side_effects=True, vmem_limit_bytes=FUSED_VMEM
        ),
    )(
        queries.reshape(own_rows, dim),
        cand_ids[:, 0],
        owner_map,
        teacher[:, 0],
        jnp.transpose(weights),
        lengths.reshape(1, block),
        jnp.transpose(passages[:, 0], (1, 0, 2)),
    )
    passage_grad, query_grad, loss = pl.pallas_call(
        finish_kernel,
        name="finish",
        out_shape=[
            jax.ShapeDtypeStruct((tokens, block, dim), bf16),
            jax.ShapeDtypeStruct((own_rows, dim), f32),
            jax.ShapeDtypeStruct((1, 1), f32),
        ],
        in_specs=[VMEM_SPEC] * 2,
        out_specs=[anywhere] * 3,
        scratch_shapes=[vmem((1, 1), f32), dma((pieces + 2,))],
    )(*(pltpu.with_memory_space_constraint(x, pltpu.VMEM) for x in results))
    return (
        loss.reshape(()),
        query_grad.reshape(count, 1, query_len, dim),
        jnp.transpose(passage_grad, (1, 0, 2))[:, None],
    )


FUSED_VMEM = 52 * 2**20


def fits(groups, queries, passages):
    width = groups * queries.shape[0] * queries.shape[2]
    block, _, tokens, dim = passages.shape
    need = tokens * width * (2 * block + 4 * 16) + 10 * tokens * block * dim
    need += 8 * width * (2 * block + 2 * dim)
    whole = groups & (groups - 1) == 0 and groups > 1 and width % (2 * LANES) == 0
    return whole and 2 * block == LANES and dim == LANES and tokens <= 256 and need < FUSED_VMEM


def step(*args):
    if fits(lax.axis_size("grp"), args[0], args[1]):
        return fused(*args)
    return on_device(*args)


def solution(mesh):
    return jax.shard_map(
        step,
        mesh=mesh,
        in_specs=(
            P("grp", "rep", None, None),
            P("grp", "rep", None, None),
            P("grp", "rep"),
            P("grp", "rep", None),
            P("rep", None),
            P("grp", "rep", None),
            P("grp", "rep"),
        ),
        out_specs=(P(), P("grp", "rep", None, None), P("grp", "rep", None, None)),
        check_vma=False,
    )
```

```python
import functools
import math

import jax
import jax.numpy as jnp
from jax import lax
from jax.experimental import pallas as pl
from jax.experimental.pallas import tpu as pltpu
from jax.sharding import PartitionSpec as P

temper = 0.05
to_base2 = 1.0 / (temper * math.log(2.0))
LANES = 128
MESH = pl.DeviceIdType.MESH
HIGH = lax.Precision.HIGHEST
VMEM_SPEC = pl.BlockSpec(memory_space=pltpu.VMEM)


def greet(groups, replicas, me, mine):
    barrier = pltpu.get_barrier_semaphore()
    for step in range(1, groups):
        pl.semaphore_signal(
            barrier, inc=1, device_id={"grp": lax.rem(me + step, groups)}, device_id_type=MESH
        )
    for step in range(1, replicas):
        pl.semaphore_signal(
            barrier, inc=1, device_id={"rep": lax.rem(mine + step, replicas)}, device_id_type=MESH
        )


def greeted(groups, replicas):
    pl.semaphore_wait(pltpu.get_barrier_semaphore(), groups - 1 + replicas - 1)


def share_kernel(
    groups, block, queries_ref, cand_ref, map_ref, teacher_ref, weights_ref,
    all_queries, all_meta, query_buf, meta_buf, send_sem, recv_sem,
):
    me = lax.axis_index("grp")
    greet(groups, 1, me, 0)
    count, ways = cand_ref.shape
    table = map_ref[...].astype(jnp.float32)
    ids = lax.broadcasted_iota(jnp.int32, (ways, table.shape[1]), 1)
    diagonal = lax.broadcasted_iota(jnp.int32, (ways, ways), 0) == lax.broadcasted_iota(
        jnp.int32, (ways, ways), 1
    )
    teacher = teacher_ref[...]
    top = jnp.max(teacher, axis=1, keepdims=True)
    log_teacher = teacher - top
    log_teacher = log_teacher - jnp.log(jnp.sum(jnp.exp(log_teacher), axis=1, keepdims=True))
    prob = jnp.exp(log_teacher)
    entropy = jnp.sum(prob * log_teacher, axis=1, keepdims=True)
    meta_buf[me] = jnp.zeros(meta_buf.shape[1:], jnp.float32)
    for q in range(count):
        line = cand_ref[q : q + 1, :].astype(jnp.float32)
        column = jnp.sum(jnp.where(diagonal, line, 0.0), axis=1, keepdims=True).astype(jnp.int32)
        row = jnp.sum(jnp.where(column == ids, table, 0.0), axis=1, keepdims=True)
        row = jnp.sum(jnp.where(diagonal, row, 0.0), axis=0, keepdims=True)
        meta_buf[me, q : q + 1, :ways] = row
    meta_buf[me, count : 2 * count, :ways] = prob
    for q in range(count):
        meta_buf[me, 2 * count + q : 2 * count + q + 1, :] = jnp.broadcast_to(
            weights_ref[:, q : q + 1], (1, LANES)
        )
    meta_buf[me, 3 * count : 4 * count, :] = jnp.broadcast_to(entropy, (count, LANES))
    query_buf[me] = queries_ref[...]
    greeted(groups, 1)
    copies = []
    for step in range(1, groups):
        peer = lax.rem(me + step, groups)
        for which, buf in enumerate((query_buf, meta_buf)):
            copies.append(
                pltpu.make_async_remote_copy(
                    src_ref=buf.at[me],
                    dst_ref=buf.at[me],
                    send_sem=send_sem.at[which, step],
                    recv_sem=recv_sem.at[which, step],
                    device_id={"grp": peer},
                    device_id_type=MESH,
                )
            )
            copies[-1].start()
    for copy in copies:
        copy.wait()
    all_queries[...] = query_buf[...]
    all_meta[...] = meta_buf[...]


def span_of(tokens, limit):
    return max(size for size in range(1, limit + 1) if tokens % size == 0)


def lengths_of(lengths_ref, first, rows, width):
    index = lax.broadcasted_iota(jnp.int32, (rows, width), 0)
    found = jnp.zeros((rows, width), jnp.int32)
    for k in range(rows):
        found = jnp.where(index == k, lengths_ref[first + k], found)
    return found


def forward_kernel(
    count, ways, block, lengths_ref, passages_ref, queries_ref, meta_ref,
    lse_ref, score_ref, hits_ref, mass_ref, held, all_lse,
):
    step = pl.program_id(0)
    part = pl.program_id(1)
    groups = meta_ref.shape[0]
    tokens, rows, dim = passages_ref.shape
    width = queries_ref.shape[0]
    slot = score_ref.shape[1]

    @pl.when((step == 0) & (part == 0))
    def _():
        spots = lax.broadcasted_iota(jnp.int32, (ways, groups * slot), 1)
        for source in range(groups):
            turned = jnp.transpose(meta_ref[source])
            for q in range(count):
                row = turned[:ways, q : q + 1].astype(jnp.int32)
                spot = row + (slot - block) * (row // block)
                hot = spot == spots
                place = source * count + q
                hits_ref[place : place + 1, :] = jnp.sum(
                    jnp.where(hot, 1.0, 0.0), axis=0, keepdims=True
                )
                mass_ref[place : place + 1, :] = jnp.sum(
                    jnp.where(hot, turned[:ways, count + q : count + q + 1], 0.0),
                    axis=0,
                    keepdims=True,
                )

    lengths = lengths_of(lengths_ref, step * rows, rows, width)
    size = span_of(tokens, 20)
    highest = jnp.full((rows, width), -1e30, jnp.float32)
    for first in range(0, tokens, size):
        products = lax.dot_general(
            passages_ref[first : first + size].reshape(size * rows, dim), queries_ref[...],
            (((1,), (1,)), ((), ())), preferred_element_type=jnp.float32,
        )
        for j in range(size):
            scaled = jnp.where(
                first + j < lengths, products[j * rows : (j + 1) * rows] * to_base2, -1e30
            )
            held[first + j] = scaled
            highest = jnp.maximum(highest, scaled)
    summed = jnp.zeros((rows, width), jnp.float32)
    for j in range(tokens):
        summed = summed + jnp.exp2(held[j] - highest)
    lse = highest + jnp.log2(summed)
    lse_ref[...] = lse
    all_lse[step, part] = lse

    @pl.when((step == pl.num_programs(0) - 1) & (part == pl.num_programs(1) - 1))
    def _():
        total = score_ref.shape[0]
        parts = all_lse.shape[1]
        each = width * parts // total
        score_ref[...] = jnp.zeros_like(score_ref)
        belongs = lax.broadcasted_iota(jnp.int32, (total // parts, width), 1) // each
        pick = jnp.where(
            belongs == lax.broadcasted_iota(jnp.int32, (total // parts, width), 0), 1.0, 0.0
        )
        span = total // parts
        for k in range(parts):
            matched = jnp.concatenate(
                [all_lse[i, k] for i in range(all_lse.shape[0])], axis=0
            ) * (1.0 / to_base2)
            score_ref[k * span : (k + 1) * span, :block] = lax.dot_general(
                pick, matched, (((1,), (1,)), ((), ())),
                precision=HIGH, preferred_element_type=jnp.float32,
            )


def grade_kernel(
    groups, replicas, score_ref, hits_ref, mass_ref, meta_ref, grad_ref, loss_ref,
    score_buf, weight_buf, grad_buf, query_weight, query_entropy,
    send_sem, recv_sem, wsend_sem, wrecv_sem,
):
    me = lax.axis_index("grp")
    mine = lax.axis_index("rep")
    greet(groups, replicas, me, mine)
    total, slot = score_ref.shape
    count = total // groups
    for source in range(groups):
        span = slice(source * count, (source + 1) * count)
        query_weight[span, :] = meta_ref[source, 2 * count : 3 * count, :]
        query_entropy[span, :] = meta_ref[source, 3 * count : 4 * count, :]
    weights = query_weight[:, :1]
    score_buf[me] = score_ref[...]
    weight_buf[mine] = jnp.broadcast_to(
        jnp.sum(query_weight[...], axis=0, keepdims=True), weight_buf.shape[1:]
    )
    greeted(groups, replicas)
    copies = []
    for step in range(1, groups):
        copies.append(
            pltpu.make_async_remote_copy(
                src_ref=score_buf.at[me],
                dst_ref=score_buf.at[me],
                send_sem=send_sem.at[step],
                recv_sem=recv_sem.at[step],
                device_id={"grp": lax.rem(me + step, groups)},
                device_id_type=MESH,
            )
        )
        copies[-1].start()
    for step in range(1, replicas):
        copies.append(
            pltpu.make_async_remote_copy(
                src_ref=weight_buf.at[mine],
                dst_ref=weight_buf.at[mine],
                send_sem=wsend_sem.at[step],
                recv_sem=wrecv_sem.at[step],
                device_id={"rep": lax.rem(mine + step, replicas)},
                device_id_type=MESH,
            )
        )
        copies[-1].start()
    for copy in copies:
        copy.wait()
    weight_sum = jnp.sum(weight_buf[...], axis=0)[:1, :1]
    scores = jnp.concatenate([score_buf[owner] for owner in range(groups)], axis=1)
    hits = hits_ref[...]
    mass = mass_ref[...]
    asked = hits > 0.0
    held = jnp.where(asked, scores, -1e30)
    highest = jnp.max(held, axis=1, keepdims=True)
    summed = jnp.sum(hits * jnp.exp(held - highest), axis=1, keepdims=True)
    log_student = jnp.where(asked, scores - (highest + jnp.log(summed)), -1e30)
    student = hits * jnp.exp(log_student)
    crossed = jnp.sum(jnp.where(asked, mass * log_student, 0.0), axis=1, keepdims=True)
    divergence = query_entropy[:, :1] - crossed
    grad_buf[...] = (total * replicas) * weights / weight_sum * (student - mass)
    own = grad_buf[:, pl.ds(pl.multiple_of(me * slot, slot), slot)]
    width = grad_ref.shape[1]
    each = width // total
    belongs = lax.broadcasted_iota(jnp.int32, (total, width), 1) // each
    pick = jnp.where(belongs == lax.broadcasted_iota(jnp.int32, (total, width), 0), 1.0, 0.0)
    spread = lax.dot_general(
        own, pick, (((0,), (0,)), ((), ())), precision=HIGH, preferred_element_type=jnp.float32
    )
    grad_ref[...] = spread[: grad_ref.shape[0]]
    loss_ref[...] = jnp.broadcast_to(
        jnp.sum(weights * divergence, axis=0, keepdims=True) / weight_sum, loss_ref.shape
    )


def backward_kernel(
    lengths_ref, passages_ref, queries_ref, lse_ref, grad_ref, out_ref, partial_ref,
    total, token_total,
):
    step = pl.program_id(0)
    part = pl.program_id(1)
    parts = total.shape[0]
    tokens, rows, dim = passages_ref.shape
    width = queries_ref.shape[0]

    @pl.when(step == 0)
    def _():
        total[part] = jnp.zeros(total.shape[1:], jnp.float32)

    if parts > 1:

        @pl.when(part == 0)
        def _():
            token_total[...] = jnp.zeros_like(token_total)

    lengths = lengths_of(lengths_ref, step * rows, rows, width)[None]
    lse = lse_ref[...][None]
    grad = grad_ref[...][None]
    queries = queries_ref[...]
    size = span_of(tokens, 36)
    added = None
    for first in range(0, tokens, size):
        passage = passages_ref[first : first + size].reshape(size * rows, dim)
        products = lax.dot_general(
            passage, queries, (((1,), (1,)), ((), ())), preferred_element_type=jnp.float32
        ).reshape(size, rows, width)
        position = first + lax.broadcasted_iota(jnp.int32, (size, 1, 1), 0)
        powers = jnp.exp2(jnp.where(position < lengths, products * to_base2 - lse, -1e30))
        scaled_grad = (powers * grad).astype(jnp.bfloat16).reshape(size * rows, width)
        token_grad = jnp.dot(scaled_grad, queries, preferred_element_type=jnp.float32).reshape(
            size, rows, dim
        )
        if parts > 1:
            token_total[first : first + size] += token_grad
        else:
            out_ref[first : first + size] = token_grad.astype(jnp.bfloat16)
        piece = lax.dot_general(
            passage, scaled_grad, (((0,), (0,)), ((), ())), preferred_element_type=jnp.float32
        )
        added = piece if added is None else added + piece
    total[part] += added

    if parts > 1:

        @pl.when(part == parts - 1)
        def _():
            out_ref[...] = token_total[...].astype(jnp.bfloat16)

    @pl.when(step == pl.num_programs(0) - 1)
    def _():
        partial_ref[pl.ds(pl.multiple_of(part * width, width), width), :] = jnp.transpose(
            total[part]
        ).astype(partial_ref.dtype)


def collect_kernel(
    groups, replicas, partial_ref, loss_ref, grad_ref, loss_out,
    arrived, loss_buf, send_sem, recv_sem, lsend_sem, lrecv_sem,
):
    me = lax.axis_index("grp")
    mine = lax.axis_index("rep")
    greet(groups, replicas, me, mine)
    loss_buf[mine] = loss_ref[...]
    greeted(groups, replicas)
    copies = []
    for step in range(1, groups):
        peer = lax.rem(me + step, groups)
        copies.append(
            pltpu.make_async_remote_copy(
                src_ref=partial_ref.at[peer],
                dst_ref=arrived.at[me],
                send_sem=send_sem.at[step],
                recv_sem=recv_sem.at[step],
                device_id={"grp": peer},
                device_id_type=MESH,
            )
        )
        copies[-1].start()
    for step in range(1, replicas):
        copies.append(
            pltpu.make_async_remote_copy(
                src_ref=loss_buf.at[mine],
                dst_ref=loss_buf.at[mine],
                send_sem=lsend_sem.at[step],
                recv_sem=lrecv_sem.at[step],
                device_id={"rep": lax.rem(mine + step, replicas)},
                device_id_type=MESH,
            )
        )
        copies[-1].start()
    arrived[me] = partial_ref[me]
    for copy in copies:
        copy.wait()
    grad_ref[...] = jnp.sum(arrived[...].astype(jnp.float32), axis=0)
    loss_out[...] = jnp.sum(loss_buf[...], axis=0)[:1, :1]


def on_device(queries, passages, lengths, cand_ids, owner_map, teacher, weights):
    groups = lax.axis_size("grp")
    replicas = lax.axis_size("rep")
    count, _, query_len, dim = queries.shape
    block, _, tokens, _ = passages.shape
    ways = cand_ids.shape[2]
    own_rows = count * query_len
    width = groups * own_rows
    total = groups * count
    slot = -(-block // LANES) * LANES
    f32 = jnp.float32
    dma = pltpu.SemaphoreType.DMA
    meta_rows = -(-4 * count // 8) * 8
    all_queries, all_meta = pl.pallas_call(
        functools.partial(share_kernel, groups, block),
        name="share",
        out_shape=[
            jax.ShapeDtypeStruct((groups, own_rows, dim), queries.dtype),
            jax.ShapeDtypeStruct((groups, meta_rows, LANES), f32),
        ],
        in_specs=[VMEM_SPEC] * 5,
        out_specs=[VMEM_SPEC] * 2,
        scratch_shapes=[
            pltpu.VMEM((groups, own_rows, dim), queries.dtype),
            pltpu.VMEM((groups, meta_rows, LANES), f32),
            dma((2, groups)),
            dma((2, groups)),
        ],
        compiler_params=pltpu.CompilerParams(collective_id=0, has_side_effects=True),
    )(
        queries.reshape(own_rows, dim),
        cand_ids[:, 0],
        owner_map,
        teacher[:, 0],
        jnp.transpose(weights),
    )
    flat_queries = all_queries.reshape(width, dim)
    flat_passages = jnp.transpose(passages[:, 0], (1, 0, 2))
    flat_lengths = lengths.reshape(block)
    rows = 16 if block % 16 == 0 else block
    chunk = width if width <= 512 else width // (width // 512)
    parts = width // chunk
    grid = (block // rows, parts)
    whole = lambda *shape: pl.BlockSpec(shape, lambda i, k, *_: (0,) * len(shape))
    passage_spec = pl.BlockSpec((tokens, rows, dim), lambda i, k, *_: (0, i, 0))
    query_spec = pl.BlockSpec((chunk, dim), lambda i, k, *_: (k, 0))
    row_spec = pl.BlockSpec((rows, chunk), lambda i, k, *_: (i, k))
    both = pltpu.CompilerParams(dimension_semantics=("arbitrary", "arbitrary"))
    lse, score, hits, mass = pl.pallas_call(
        functools.partial(forward_kernel, count, ways, block),
        name="forward",
        grid_spec=pltpu.PrefetchScalarGridSpec(
            num_scalar_prefetch=1,
            grid=grid,
            in_specs=[passage_spec, query_spec, whole(groups, meta_rows, LANES)],
            out_specs=[
                row_spec,
                whole(total, slot),
                whole(total, groups * slot),
                whole(total, groups * slot),
            ],
            scratch_shapes=[
                pltpu.VMEM((tokens, rows, chunk), f32),
                pltpu.VMEM((*grid, rows, chunk), f32),
            ],
        ),
        out_shape=[
            jax.ShapeDtypeStruct((block, width), f32),
            jax.ShapeDtypeStruct((total, slot), f32),
            jax.ShapeDtypeStruct((total, groups * slot), f32),
            jax.ShapeDtypeStruct((total, groups * slot), f32),
        ],
        compiler_params=both,
    )(flat_lengths, flat_passages, flat_queries, all_meta)
    grad, loss_part = pl.pallas_call(
        functools.partial(grade_kernel, groups, replicas),
        name="grade",
        out_shape=[
            jax.ShapeDtypeStruct((block, width), f32),
            jax.ShapeDtypeStruct((8, LANES), f32),
        ],
        in_specs=[VMEM_SPEC] * 4,
        out_specs=[VMEM_SPEC] * 2,
        scratch_shapes=[
            pltpu.VMEM((groups, total, slot), f32),
            pltpu.VMEM((replicas, 8, LANES), f32),
            pltpu.VMEM((total, groups * slot), f32),
            pltpu.VMEM((total, LANES), f32),
            pltpu.VMEM((total, LANES), f32),
            dma((groups,)),
            dma((groups,)),
            dma((replicas,)),
            dma((replicas,)),
        ],
        compiler_params=pltpu.CompilerParams(collective_id=1, has_side_effects=True),
    )(score, hits, mass, all_meta)
    passage_grad, partial = pl.pallas_call(
        backward_kernel,
        name="backward",
        grid_spec=pltpu.PrefetchScalarGridSpec(
            num_scalar_prefetch=1,
            grid=grid,
            in_specs=[passage_spec, query_spec, row_spec, row_spec],
            out_specs=[passage_spec, whole(width, dim)],
            scratch_shapes=[
                pltpu.VMEM((parts, dim, chunk), f32),
                pltpu.VMEM((tokens, rows, dim) if parts > 1 else (8, rows, dim), f32),
            ],
        ),
        out_shape=[
            jax.ShapeDtypeStruct((tokens, block, dim), jnp.bfloat16),
            jax.ShapeDtypeStruct((width, dim), jnp.bfloat16),
        ],
        compiler_params=both,
    )(flat_lengths, flat_passages, flat_queries, lse, grad)
    query_grad, loss = pl.pallas_call(
        functools.partial(collect_kernel, groups, replicas),
        name="collect",
        out_shape=[
            jax.ShapeDtypeStruct((own_rows, dim), f32),
            jax.ShapeDtypeStruct((1, 1), f32),
        ],
        in_specs=[VMEM_SPEC] * 2,
        out_specs=[VMEM_SPEC] * 2,
        scratch_shapes=[
            pltpu.VMEM((groups, own_rows, dim), jnp.bfloat16),
            pltpu.VMEM((replicas, 8, LANES), f32),
            dma((groups,)),
            dma((groups,)),
            dma((replicas,)),
            dma((replicas,)),
        ],
        compiler_params=pltpu.CompilerParams(collective_id=2, has_side_effects=True),
    )(partial.reshape(groups, own_rows, dim), loss_part)
    return (
        loss.reshape(()),
        query_grad.reshape(count, 1, query_len, dim),
        jnp.transpose(passage_grad, (1, 0, 2))[:, None],
    )


def partner(me, turn):
    peer = me
    bit = 1
    while bit <= turn:
        if turn & bit:
            peer = peer + bit * (1 - 2 * lax.rem(lax.div(me, bit), 2))
        bit *= 2
    return peer


def share_meta(me, cand, table, teacher, weights, meta_buf):
    count, ways = cand.shape
    ids = lax.broadcasted_iota(jnp.int32, (ways, table.shape[1]), 1)
    diagonal = lax.broadcasted_iota(jnp.int32, (ways, ways), 0) == lax.broadcasted_iota(
        jnp.int32, (ways, ways), 1
    )
    top = jnp.max(teacher, axis=1, keepdims=True)
    log_teacher = teacher - top
    log_teacher = log_teacher - jnp.log(jnp.sum(jnp.exp(log_teacher), axis=1, keepdims=True))
    prob = jnp.exp(log_teacher)
    entropy = jnp.sum(prob * log_teacher, axis=1, keepdims=True)
    meta_buf[me] = jnp.zeros(meta_buf.shape[1:], jnp.float32)
    for q in range(count):
        line = cand[q : q + 1, :].astype(jnp.float32)
        column = jnp.sum(jnp.where(diagonal, line, 0.0), axis=1, keepdims=True).astype(jnp.int32)
        row = jnp.sum(jnp.where(column == ids, table, 0.0), axis=1, keepdims=True)
        row = jnp.sum(jnp.where(diagonal, row, 0.0), axis=0, keepdims=True)
        meta_buf[me, q : q + 1, :ways] = row
    meta_buf[me, count : 2 * count, :ways] = prob
    for q in range(count):
        meta_buf[me, 2 * count + q : 2 * count + q + 1, :] = jnp.broadcast_to(
            weights[:, q : q + 1], (1, LANES)
        )
    meta_buf[me, 3 * count : 4 * count, :] = jnp.broadcast_to(entropy, (count, LANES))


def place_candidates(count, ways, meta_ref, hits_ref, mass_ref):
    groups = meta_ref.shape[0]
    spots = lax.broadcasted_iota(jnp.int32, (ways, hits_ref.shape[1]), 1)
    for source in range(groups):
        turned = jnp.transpose(meta_ref[source])
        for q in range(count):
            hot = turned[:ways, q : q + 1].astype(jnp.int32) == spots
            place = source * count + q
            hits_ref[place : place + 1, :] = jnp.sum(
                jnp.where(hot, 1.0, 0.0), axis=0, keepdims=True
            )
            mass_ref[place : place + 1, :] = jnp.sum(
                jnp.where(hot, turned[:ways, count + q : count + q + 1], 0.0),
                axis=0,
                keepdims=True,
            )


def fused_kernel(
    groups, replicas,
    queries_hbm, cand_hbm, map_hbm, teacher_hbm, weights_hbm, lengths_hbm, passages_hbm,
    out_ref, grad_ref,
    raw, doubled, cleared, turned_ref, tops, scales, limits, held, power, inverse, lse, query_buf, folded, meta_buf,
    hits_ref, mass_ref, pick_ref, score_buf, weight_buf, grade_buf, query_weight, query_entropy,
    partial_buf, arrived, loss_buf, cand_ref, map_ref, teacher_ref, weights_ref, lengths_ref,
    load_sem, small_sem, send_sem, recv_sem, wsend_sem, wrecv_sem,
):
    f32, bf16 = jnp.float32, jnp.bfloat16
    me = lax.axis_index("grp")
    mine = lax.axis_index("rep")
    greet(groups, replicas, me, mine)
    tokens, block, dim = raw.shape
    count, ways = cand_ref.shape
    own_rows = query_buf.shape[1]
    width = groups * own_rows
    half = width // 2
    total = groups * count
    rows = held.shape[2]
    blocks = block // rows
    own_copy = pltpu.make_async_copy(queries_hbm, query_buf.at[0], small_sem.at[0])
    own_copy.start()
    loads = []
    pieces = load_sem.shape[0]
    for k in range(pieces):
        at = pl.ds(k * (tokens // pieces), tokens // pieces)
        loads.append(pltpu.make_async_copy(passages_hbm.at[at], raw.at[at], load_sem.at[k]))
    small = []
    for k, (there, here) in enumerate(
        (
            (cand_hbm, cand_ref), (map_hbm, map_ref), (teacher_hbm, teacher_ref),
            (weights_hbm, weights_ref), (lengths_hbm, lengths_ref),
        )
    ):
        small.append(pltpu.make_async_copy(there, here, small_sem.at[1 + k]))
    for copy in small + loads:
        copy.start()

    def exchange(source, target, which, turns):
        copies = {}
        for turn in turns:
            copies[turn] = pltpu.make_async_remote_copy(
                src_ref=source(turn),
                dst_ref=target(turn),
                send_sem=send_sem.at[which, turn],
                recv_sem=recv_sem.at[which, turn],
                device_id={"grp": partner(me, turn)},
                device_id_type=MESH,
            )
            copies[turn].start()
        return copies

    def across(buf, which):
        copies = []
        for step in range(1, replicas):
            copies.append(
                pltpu.make_async_remote_copy(
                    src_ref=buf.at[mine],
                    dst_ref=buf.at[mine],
                    send_sem=wsend_sem.at[which, step],
                    recv_sem=wrecv_sem.at[which, step],
                    device_id={"rep": lax.rem(mine + step, replicas)},
                    device_id_type=MESH,
                )
            )
            copies[-1].start()
        return copies

    near = range(1, groups)
    far = range(groups - 1, 0, -1)
    own_copy.wait()
    greeted(groups, replicas)
    query_copies = exchange(lambda _: query_buf.at[0], lambda t: query_buf.at[t], 0, near)

    for copy in small:
        copy.wait()
    share_meta(
        me, cand_ref[...], map_ref[...].astype(f32), teacher_ref[...], weights_ref[...], meta_buf
    )
    meta_copies = exchange(lambda _: meta_buf.at[me], lambda _: meta_buf.at[me], 1, far)

    wide = jnp.transpose(
        jnp.broadcast_to(lengths_ref[...].astype(f32), (LANES, lengths_ref.shape[1]))
    )
    wide16 = wide.astype(bf16)
    column = lax.broadcasted_iota(jnp.int32, (1, width), 1)
    each = own_rows // count
    turn = column // own_rows
    source = jnp.zeros_like(turn)
    for k in range(groups):
        source = jnp.where(turn == k, partner(me, k), source)
    query = source * count + (column - turn * own_rows) // each
    pick = jnp.where(query == lax.broadcasted_iota(jnp.int32, (total, width), 0), 1.0, 0.0)
    pick_ref[...] = pick
    for copy in loads:
        copy.wait()
    first_token = raw[0]
    prep = span_of(tokens, 12)

    def prepare(k, _):
        for j in range(prep):
            at = k * prep + j
            here = raw[at]
            usable = at.astype(f32).astype(bf16) < wide16
            known = jnp.where(usable, here, first_token)
            doubled[:, at] = known.reshape(blocks, rows, dim)
            cleared[:, at] = jnp.where(usable, here, jnp.zeros_like(here)).reshape(
                blocks, rows, dim
            )
        return 0

    lax.fori_loop(0, tokens // prep, prepare, 0)

    single = jnp.minimum(me + 1, 1)
    bite = span_of(tokens, 180)
    units = [(h, b) for h in range(2) for b in range(blocks)]

    def forward(u):
        ahead = units[u] if u < len(units) else None
        behind = units[u - 1] if u > 0 else None
        highest = None
        if ahead is not None:
            h, b = ahead
            left = doubled[b].reshape(tokens * rows, dim)
            products = lax.dot_general(
                jnp.concatenate([left, left], axis=1), folded[h],
                (((1,), (1,)), ((), ())), preferred_element_type=f32,
            ).reshape(tokens, rows, half)
        if behind is not None:
            h0, b0 = behind
            above = tops[(u - 1) % 2]
            sums = [None] * 2
        peaks = [None] * 2
        for first in range(tokens // 2):
            for line in range(2):
                j = line * (tokens // 2) + first
                if ahead is not None:
                    held[u % 2, j] = products[j]
                    peaks[line] = products[j] if first == 0 else jnp.maximum(peaks[line], products[j])
                if behind is not None:
                    powers = jnp.exp2(held[(u - 1) % 2, j] - above)
                    power[h0, b0, j] = powers.astype(bf16)
                    sums[line] = powers if first == 0 else sums[line] + powers
        if ahead is not None:
            highest = functools.reduce(jnp.maximum, peaks)
        if behind is not None:
            summed = functools.reduce(jnp.add, sums)
        if ahead is not None:
            tops[u % 2] = highest
        if behind is not None:
            at = slice(b0 * rows, (b0 + 1) * rows)
            to = slice(h0 * half, (h0 + 1) * half)
            unused = (tokens - limits[at, :1]) * jnp.exp2(held[(u - 1) % 2, 0] - above)
            summed = summed - unused
            lse[at, to] = above + jnp.log2(summed)
            inverse[at, to] = 1.0 / summed

    limits[...] = wide
    for u in range(len(units) + 1):
        if u < len(units) and units[u][1] == 0:
            h = units[u][0]
            span = slice(h * (groups // 2), (h + 1) * (groups // 2))
            for t in range(groups)[span]:
                if t:
                    query_copies[t].wait()
            scaled = query_buf[span].reshape(half, dim).astype(f32) * to_base2
            upper = scaled.astype(bf16)
            folded[h, :, :dim] = upper
            folded[h, :, dim:] = (scaled - upper.astype(f32)).astype(bf16)

        def trip(_, carry, u=u):
            forward(u)
            return carry

        lax.fori_loop(0, single, trip, 0)

    pick16 = pick_ref[...].astype(bf16)
    rest = lse[...] * (1.0 / to_base2)
    scores = None
    for _ in range(3):
        term = rest.astype(bf16)
        rest = rest - term.astype(f32)
        piece = lax.dot_general(
            pick16, term, (((1,), (1,)), ((), ())), preferred_element_type=f32
        )
        scores = piece if scores is None else scores + piece
    score_buf[me, :, :block] = scores[: total // 2]
    score_buf[me, :, block:] = scores[total // 2 :]
    score_copies = exchange(lambda _: score_buf.at[me], lambda _: score_buf.at[me], 2, far)
    for t in meta_copies:
        meta_copies[t].wait()
    for owner in range(groups):
        at = slice(owner * count, (owner + 1) * count)
        query_weight[at, :] = meta_buf[owner, 2 * count : 3 * count, :]
        query_entropy[at, :] = meta_buf[owner, 3 * count : 4 * count, :]
    weight_buf[mine] = jnp.broadcast_to(
        jnp.sum(query_weight[...], axis=0, keepdims=True), weight_buf.shape[1:]
    )
    weight_copies = across(weight_buf, 0)
    place_candidates(count, ways, meta_buf, hits_ref, mass_ref)
    for b in range(blocks):
        turned_ref[b] = jnp.transpose(cleared[b].reshape(tokens * rows, dim))
    for copy in weight_copies:
        copy.wait()
    weights = query_weight[:, :1]
    weight_sum = jnp.sum(weight_buf[...], axis=0)[:1, :1]
    factor = (total * replicas) * weights / weight_sum
    hits = hits_ref[...]
    mass = mass_ref[...]
    asked = hits > 0.0
    for t in score_copies:
        score_copies[t].wait()
    left = lax.broadcasted_iota(jnp.int32, (total // 2, LANES), 1) < block
    tiles = []
    for owner in range(0, groups, 2):
        one, two = score_buf[owner], score_buf[owner + 1]
        tiles.append(
            jnp.concatenate(
                [
                    jnp.where(left, one, pltpu.roll(two, block, 1)),
                    jnp.where(left, pltpu.roll(one, block, 1), two),
                ],
                axis=0,
            )
        )
    scores = jnp.concatenate(tiles, axis=1)
    masked = jnp.where(asked, scores, -1e30)
    highest = jnp.max(masked, axis=1, keepdims=True)
    summed = jnp.sum(hits * jnp.exp(masked - highest), axis=1, keepdims=True)
    log_student = jnp.where(asked, scores - (highest + jnp.log(summed)), -1e30)
    grade_buf[...] = factor * (hits * jnp.exp(log_student) - mass)
    pair = grade_buf[:, pl.ds(pl.multiple_of(lax.div(me, 2) * LANES, LANES), LANES)]
    odd = jnp.broadcast_to(lax.rem(me, 2), pair.shape) == 1
    own = jnp.where(odd, pltpu.roll(pair, block, 1), pair)[:, :block]
    upper = own.astype(bf16)
    lower = (own - upper.astype(f32)).astype(bf16)
    pick16 = pick_ref[...].astype(bf16)
    spread = lax.dot_general(
        jnp.concatenate([upper, lower], axis=0), jnp.concatenate([pick16, pick16], axis=0),
        (((0,), (0,)), ((), ())), preferred_element_type=f32,
    )
    scale = (inverse[...] * spread).astype(bf16)
    for h in range(2):
        for b in range(blocks):
            scales[h, b] = scale[b * rows : (b + 1) * rows, h * half : (h + 1) * half]

    partial_copies = {}
    for h in (1, 0):

        def backward(_, carry, h=h):
            added = None
            for b in range(blocks):
                piece = jnp.dot(
                    turned_ref[b],
                    (power[h, b] * scales[h, b][None]).reshape(tokens * rows, half),
                    preferred_element_type=f32,
                )
                added = piece if added is None else added + piece
            partial_buf[h * (groups // 2) : (h + 1) * (groups // 2)] = (
                jnp.transpose(added).astype(bf16).reshape(groups // 2, own_rows, dim)
            )
            return carry

        lax.fori_loop(0, single, backward, 0)
        span = slice(h * (groups // 2), (h + 1) * (groups // 2))
        partial_copies.update(
            exchange(
                lambda t: partial_buf.at[t], lambda t: arrived.at[t], 3,
                [t for t in range(groups)[span][::-1] if t],
            )
        )
    crossed = jnp.sum(jnp.where(asked, mass * log_student, 0.0), axis=1, keepdims=True)
    divergence = query_entropy[:, :1] - crossed
    loss_buf[mine] = jnp.broadcast_to(
        jnp.sum(weights * divergence, axis=0, keepdims=True) / weight_sum, loss_buf.shape[1:]
    )
    loss_copies = across(loss_buf, 1)

    def tokenwise(_, carry):
        for b in range(blocks):
            at = slice(b * rows, (b + 1) * rows)
            token_grad = None
            for h in range(2):
                span = slice(h * (groups // 2), (h + 1) * (groups // 2))
                piece = jnp.dot(
                    (power[h, b] * scales[h, b][None]).reshape(tokens * rows, half),
                    query_buf[span].reshape(half, dim), preferred_element_type=f32,
                )
                token_grad = piece if token_grad is None else token_grad + piece
            token_grad = token_grad.reshape(tokens, rows, dim)
            limit = limits[at].astype(bf16)
            for j in range(tokens):
                usable = jnp.full((), j, bf16) < limit
                out_ref[j, at, :] = jnp.where(
                    usable, token_grad[j].astype(bf16), jnp.zeros((rows, dim), bf16)
                )
        return carry

    lax.fori_loop(0, single, tokenwise, 0)

    for t in partial_copies:
        partial_copies[t].wait()
    for copy in loss_copies:
        copy.wait()
    grad_ref[:own_rows, :] = partial_buf[0].astype(f32) + jnp.sum(
        arrived[1:].astype(f32), axis=0
    )
    grad_ref[own_rows:, :] = jnp.sum(loss_buf[...], axis=0)


def finish_kernel(out_ref, grad_ref, out_hbm, grad_hbm, loss_hbm, loss_ref, sem):
    copies = []
    tokens = out_ref.shape[0]
    pieces = sem.shape[0] - 2
    for k in range(pieces):
        at = pl.ds(k * (tokens // pieces), tokens // pieces)
        copies.append(pltpu.make_async_copy(out_ref.at[at], out_hbm.at[at], sem.at[k]))
        copies[-1].start()
    own = grad_hbm.shape[0]
    copies.append(pltpu.make_async_copy(grad_ref.at[pl.ds(0, own)], grad_hbm, sem.at[pieces]))
    copies[-1].start()
    loss_ref[...] = grad_ref[own : own + 1, :1]
    copies.append(pltpu.make_async_copy(loss_ref, loss_hbm, sem.at[pieces + 1]))
    copies[-1].start()
    for copy in copies:
        copy.wait()


def fused(queries, passages, lengths, cand_ids, owner_map, teacher, weights):
    groups = lax.axis_size("grp")
    replicas = lax.axis_size("rep")
    count, _, query_len, dim = queries.shape
    block, _, tokens, _ = passages.shape
    ways = cand_ids.shape[2]
    own_rows = count * query_len
    width = groups * own_rows
    total = groups * count
    rows = 16
    f32, bf16, i32 = jnp.float32, jnp.bfloat16, jnp.int32
    dma = pltpu.SemaphoreType.DMA
    meta_rows = -(-4 * count // 8) * 8
    vmem = pltpu.VMEM
    anywhere = pl.BlockSpec(memory_space=pl.ANY)
    pieces = span_of(tokens, 5)
    results = pl.pallas_call(
        functools.partial(fused_kernel, groups, replicas),
        name="fused",
        out_shape=[
            vmem((tokens, block, dim), bf16),
            vmem((own_rows + 8, dim), f32),
        ],
        in_specs=[anywhere] * 7,
        out_specs=[VMEM_SPEC] * 2,
        scratch_shapes=[
            vmem((tokens, block, dim), bf16),
            vmem((block // rows, tokens, rows, dim), bf16),
            vmem((block // rows, tokens, rows, dim), bf16),
            vmem((block // rows, dim, tokens * rows), bf16),
            vmem((2, rows, width // 2), f32),
            vmem((2, block // rows, rows, width // 2), bf16),
            vmem((block, LANES), f32),
            vmem((2, tokens, rows, width // 2), f32),
            vmem((2, block // rows, tokens, rows, width // 2), bf16),
            vmem((block, width), f32),
            vmem((block, width), f32),
            vmem((groups, own_rows, dim), bf16),
            vmem((2, width // 2, 2 * dim), bf16),
            vmem((groups, meta_rows, LANES), f32),
            vmem((total, groups * block), f32),
            vmem((total, groups * block), f32),
            vmem((total, width), f32),
            vmem((groups, total // 2, LANES), f32),
            vmem((replicas, 8, LANES), f32),
            vmem((total, groups * block), f32),
            vmem((total, LANES), f32),
            vmem((total, LANES), f32),
            vmem((groups, own_rows, dim), bf16),
            vmem((groups, own_rows, dim), bf16),
            vmem((replicas, 8, LANES), f32),
            vmem((count, ways), i32),
            vmem((1, groups * block), i32),
            vmem((count, ways), f32),
            vmem((1, count), f32),
            vmem((1, block), i32),
            dma((pieces,)),
            dma((6,)),
            dma((4, groups)),
            dma((4, groups)),
            dma((2, replicas)),
            dma((2, replicas)),
        ],
        compiler_params=pltpu.CompilerParams(
            collective_id=3, has_side_effects=True, vmem_limit_bytes=FUSED_VMEM,
        ),
    )(
        queries.reshape(own_rows, dim),
        cand_ids[:, 0],
        owner_map,
        teacher[:, 0],
        jnp.transpose(weights),
        lengths.reshape(1, block),
        jnp.transpose(passages[:, 0], (1, 0, 2)),
    )
    passage_grad, query_grad, loss = pl.pallas_call(
        finish_kernel,
        name="finish",
        out_shape=[
            jax.ShapeDtypeStruct((tokens, block, dim), bf16),
            jax.ShapeDtypeStruct((own_rows, dim), f32),
            jax.ShapeDtypeStruct((1, 1), f32),
        ],
        in_specs=[VMEM_SPEC] * 2,
        out_specs=[anywhere] * 3,
        scratch_shapes=[vmem((1, 1), f32), dma((pieces + 2,))],
    )(*(pltpu.with_memory_space_constraint(x, pltpu.VMEM) for x in results))
    return (
        loss.reshape(()),
        query_grad.reshape(count, 1, query_len, dim),
        jnp.transpose(passage_grad, (1, 0, 2))[:, None],
    )


FUSED_VMEM = 52 * 2**20


def fits(groups, queries, passages):
    width = groups * queries.shape[0] * queries.shape[2]
    block, _, tokens, dim = passages.shape
    need = tokens * width * (2 * block + 4 * 16) + 10 * tokens * block * dim
    need += 8 * width * (2 * block + 2 * dim)
    whole = groups & (groups - 1) == 0 and groups > 1 and width % (2 * LANES) == 0
    return whole and 2 * block == LANES and dim == LANES and tokens <= 256 and need < FUSED_VMEM


def step(*args):
    if fits(lax.axis_size("grp"), args[0], args[1]):
        return fused(*args)
    return on_device(*args)


def solution(mesh):
    return jax.shard_map(
        step,
        mesh=mesh,
        in_specs=(
            P("grp", "rep", None, None),
            P("grp", "rep", None, None),
            P("grp", "rep"),
            P("grp", "rep", None),
            P("rep", None),
            P("grp", "rep", None),
            P("grp", "rep"),
        ),
        out_specs=(P(), P("grp", "rep", None, None), P("grp", "rep", None, None)),
        check_vma=False,
    )
```
